32 devices in a mesh: tissue: 2 (over core), row: 4 (over y, x), col: 4 (over z).
Axes of the slice: x: 2, y: 2, z: 4, core: 2. Of those that a mesh axis runs over, the one named last changes fastest.
Arguments:
- expr: float32 [1200, 16384], P(('tissue', 'row'), 'col'), parts along dimension 0, may hold values from -48 to 88
- win_genes: int32 [256], replicated, may hold values from 0 to 16383, as said below
Outputs:
- margin: float32 [512, 16384], P(('tissue', 'row'), 'col'), parts along dimension 0
- degree: float32 [32768], P(('tissue', 'col')), parts along dimension 0
The draws below stay inside these ranges and needn't reach their ends.
There are 2 independent parts, one for each index of `tissue`. The reference program is written for one: setup_inputs(seed, part) draws one part's arguments, and reference() takes and returns one part's arrays. A program takes and returns all parts, laid end to end along the dimension named above; an argument that names none is the same for every part. Nothing has to cross between parts.
Inputs may be any that keep to these rules, and one draw needn't show every extreme that they name: `win_genes`: 256 distinct gene numbers.
All inputs are finite; a program needn't handle non-finite values.
Results may differ from the reference program's by a relative error of at most 0.00077.
Values may be sent and summed in bfloat16 or wider, within the bound.
A program may use at most 128 MiB of HBM per device.

```python
import jax
import jax.numpy as jnp
from jax import lax

G = 16384
S = 600
WIN = 256
N_COL = 4


factor_count = 24


def draw_expr(key, part):
    keys = jax.random.split(jax.random.fold_in(key, 11), 7)
    factors = jax.random.truncated_normal(keys[0], -4.0, 4.0, (S, factor_count), jnp.float32)
    module = jax.random.randint(keys[1], (G,), 0, factor_count)
    sign = jnp.where(jax.random.randint(keys[2], (G,), 0, 2) == 0, -1.0, 1.0)
    load = jax.random.uniform(keys[3], (G,), jnp.float32, 0.4, 1.6) * sign
    loads = jax.random.normal(keys[4], (factor_count, G), jnp.float32) * 0.15
    loads = loads + jax.nn.one_hot(module, factor_count, dtype=jnp.float32).T * load[None, :]
    noise_scale = jax.random.uniform(keys[5], (G,), jnp.float32, 0.3, 1.2)
    noise = jax.random.normal(keys[6], (S, G), jnp.float32)
    signal = jnp.dot(factors, loads, precision=lax.Precision.HIGHEST) + noise * noise_scale[None, :]
    signal = jnp.clip(signal, -12.0, 12.0)
    return signal


def draw_win_genes(key, part):
    order = jax.random.permutation(jax.random.fold_in(key, 23), G)
    return order[:WIN].astype(jnp.int32)


def setup_inputs(seed: int = 0, part: int = 0) -> dict:
    streams_of = jax.random.split(jax.random.key(seed), 3)
    own_keys = jax.random.split(jax.random.fold_in(streams_of[2], part), 3)
    return {
        "expr": draw_expr(jax.random.fold_in(jax.random.fold_in(streams_of[2], part), 71), part),
        "win_genes": draw_win_genes(jax.random.fold_in(streams_of[2], 71), part),
    }


def power_eight(corr):
    half = (1.0 + corr) * 0.5
    half = half * half
    half = half * half
    return half * half

def reference(expr, win_genes):
    mean = lax.optimization_barrier(jnp.sum(expr, axis=0)) / S
    centered = expr - mean
    squares = lax.optimization_barrier(jnp.sum(centered * centered, axis=0))
    z = (centered / jnp.sqrt(squares + 1e-06)).astype(jnp.bfloat16)
    zwin = jnp.take(z, win_genes.astype(jnp.int32), axis=1)
    panel = power_eight(jnp.dot(zwin.T, z, preferred_element_type=jnp.float32)).astype(jnp.bfloat16)
    width = G // N_COL

    def column(start):
        block = lax.dynamic_slice_in_dim(z, start, width, 1)
        adj = power_eight(jnp.dot(z.T, block, preferred_element_type=jnp.float32)).astype(jnp.bfloat16)
        rows_id = jnp.arange(G, dtype=jnp.int32)
        cols_id = start + jnp.arange(width, dtype=jnp.int32)
        keep = rows_id[:, None] != cols_id[None, :]
        degree = lax.optimization_barrier(jnp.sum(jnp.where(keep, adj.astype(jnp.float32), jnp.float32(0.0)), axis=0))
        margin = jnp.dot(panel, adj, preferred_element_type=jnp.float32)
        return (margin, degree)
    starts = jnp.arange(N_COL, dtype=jnp.int32) * width
    blocks, degrees = lax.map(column, starts)
    margin = jnp.transpose(blocks, (1, 0, 2)).reshape(WIN, G)
    return (margin, degrees.reshape(G))
```

```python
import functools

import jax
import jax.numpy as jnp
from jax import lax
from jax.experimental import pallas as pl
from jax.experimental.pallas import tpu as pltpu
from jax.sharding import PartitionSpec as P

MESH = pl.DeviceIdType.MESH
F32 = jnp.float32
BF16 = jnp.bfloat16


def power_eight(corr):
    half = (1.0 + corr) * 0.5
    half = half * half
    half = half * half
    return half * half


def flip(r, d):
    out = r
    for b in range(6):
        bit = 1 << b
        out = out + ((d // bit) % 2) * (1 - 2 * ((r // bit) % 2)) * bit
    return out


def dot(a, b, dims=((1,), (0,))):
    return lax.dot_general(a, b, (dims, ((), ())), preferred_element_type=F32)


def kernel(R, C, eps, expr, win, out, dego,
           stats, zl, zcol, zrt, zw, zwr, zwt, pbuf, macc, rs, degb, degr,
           s_st, r_st, s_aa, r_aa, s_ga, r_ga, s_zc, r_zc, s_zr, r_zr,
           s_up, r_up, s_dn, r_dn, s_rs, r_rs, s_dg, r_dg):
    r = lax.axis_index("row")
    c = lax.axis_index("col")
    S, width = expr.shape
    pad = zl.shape[0]
    slab = width // R
    W = zw.shape[2]
    per = W // R
    NC, chunk = zrt.shape[1], zrt.shape[2]

    barrier = pltpu.get_barrier_semaphore()
    for d in range(1, R):
        pl.semaphore_signal(barrier, inc=1, device_id={"row": flip(r, d)}, device_id_type=MESH)
    for d in range(1, C):
        pl.semaphore_signal(barrier, inc=1, device_id={"col": lax.rem(c + d, C)}, device_id_type=MESH)

    for j in range(R):
        cols = slice(j * slab, (j + 1) * slab)
        x = expr[:, cols]
        total = jnp.sum(x, axis=0, keepdims=True)
        dev = x - total * (1.0 / S)
        stats[0, 0:1, cols] = total
        stats[0, 1:2, cols] = jnp.sum(dev * dev, axis=0, keepdims=True)
    pl.semaphore_wait(barrier, R + C - 2)

    def rowcopy(src, dst, ss, rr, d):
        return pltpu.make_async_remote_copy(
            src_ref=src, dst_ref=dst, send_sem=ss, recv_sem=rr,
            device_id={"row": flip(r, d)}, device_id_type=MESH)

    def colcopy(src, dst, ss, rr, peer):
        return pltpu.make_async_remote_copy(
            src_ref=src, dst_ref=dst, send_sem=ss, recv_sem=rr,
            device_id={"col": peer}, device_id_type=MESH)

    st = [rowcopy(stats.at[0], stats.at[d], s_st.at[d], r_st.at[d], d) for d in range(1, R)]
    for cp in st:
        cp.start()
    macc[...] = jnp.zeros_like(macc)
    zl[pad - 16:pad, :] = jnp.zeros((16, width), BF16)
    pbuf[...] = jnp.ones_like(pbuf)
    for cp in st:
        cp.wait_recv()

    for j in range(R):
        cols = slice(j * slab, (j + 1) * slab)
        total = stats[0, 0:1, cols]
        for d in range(1, R):
            total = total + stats[d, 0:1, cols]
        mean = total / (S * R)
        sq = jnp.zeros_like(mean)
        for d in range(R):
            gap = stats[d, 0:1, cols] * (1.0 / S) - mean
            sq = sq + (stats[d, 1:2, cols] + S * gap * gap)
        inv = 1.0 / jnp.sqrt(sq + eps)
        zl[0:S, cols] = ((expr[:, cols] - mean) * inv).astype(BF16)

    mine = pl.ds(pl.multiple_of(r * pad, 16), pad)
    aa = []
    for k in range(NC):
        for d in range(1, R):
            q = flip(r, d)
            at = pl.multiple_of(q * slab + k * chunk, 128)
            aa.append(rowcopy(zl.at[:, pl.ds(at, chunk)],
                              zcol.at[q, mine, k * chunk:(k + 1) * chunk],
                              s_aa.at[k, d], r_aa.at[k, d], d))
            aa[-1].start()
    zcol[r, mine, :] = zl[:, pl.ds(pl.multiple_of(r * slab, 128), slab)]

    pick = jnp.zeros((pad, W), F32)
    for j in range(R):
        gene = lax.broadcasted_iota(jnp.int32, (slab, W), 0) + (c * width + j * slab)
        onehot = jnp.where(gene == win[...], 1.0, 0.0).astype(BF16)
        pick = pick + dot(zl[:, j * slab:(j + 1) * slab], onehot)
    zw[0] = pick.astype(BF16)
    zc = []
    for d in range(1, C):
        zc.append(colcopy(zw.at[0], zw.at[d], s_zc.at[d], r_zc.at[d], lax.rem(c + d, C)))
        zc[-1].start()

    zr_own = zcol.at[r]
    lo, hi = c > 0, c < C - 1

    def up(s, k):
        i = c - s
        return colcopy(zrt.at[i, k], zrt.at[i, k], s_up.at[s, k], r_up.at[s, k], c + 1)

    def up_in(s, k):
        i = c - s
        return colcopy(zrt.at[i, k], zrt.at[i, k], s_up.at[s - 1, k], r_up.at[s - 1, k], c + 1)

    def down(s, k):
        i = c + s
        return colcopy(zrt.at[i, k], zrt.at[i, k], s_dn.at[s, k], r_dn.at[s, k], c - 1)

    def down_in(s, k):
        i = c + s
        return colcopy(zrt.at[i, k], zrt.at[i, k], s_dn.at[s - 1, k], r_dn.at[s - 1, k], c - 1)

    for k in range(NC):
        for cp in aa[k * (R - 1):(k + 1) * (R - 1)]:
            cp.wait_recv()
        zrt[c, k] = zr_own[:, k * chunk:(k + 1) * chunk].T

        @pl.when(hi)
        def _():
            up(0, k).start()

        @pl.when(lo)
        def _():
            down(0, k).start()

    relay = R == 4

    def gather(k, d):
        piece = zcol.at[r, :, pl.ds(pl.multiple_of(k * chunk, 128), chunk)]
        return rowcopy(piece, piece, s_ga.at[k, d], r_ga.at[k, d], d)

    def forward(k, via, to):
        piece = zcol.at[flip(r, via), :, pl.ds(pl.multiple_of(k * chunk, 128), chunk)]
        return rowcopy(piece, piece, s_ga.at[k, R - 1], r_ga.at[k, R - 1], to)

    direct = R - 1 if relay else R
    for d in range(1, direct):
        gather(0, d).start()

    tot = zw[0].astype(F32)
    for cp in zc:
        cp.wait_recv()
    for d in range(1, C):
        tot = tot + zw[d].astype(F32)
    zwr[0] = tot.astype(BF16)
    zr = []
    for d in range(1, R):
        zr.append(rowcopy(zwr.at[0], zwr.at[d], s_zr.at[d], r_zr.at[d], d))
        zr[-1].start()
    for k in range(1, NC):
        for d in range(1, direct):
            gather(k, d).start()
    for cp in zr:
        cp.wait_recv()
    for d in range(R):
        zwt[pl.ds(pl.multiple_of(flip(r, d) * pad, 16), pad), :] = zwr[d]

    def compute(i, k, d_lo, d_hi):
        def one(d, _):
            j = flip(r, d)
            adj = power_eight(dot(zrt[i, k], zcol[j])).astype(BF16)
            macc[j] += dot(pbuf[i, k], adj)
            return 0
        lax.fori_loop(d_lo, d_hi, one, 0)

    def panel(i, k):
        pt = power_eight(dot(zrt[i, k], zwt[...])).T
        pbuf[i, k, 0:W, :] = pt.astype(BF16)

    def arrive(s, k):
        @pl.when(c - s >= 0)
        def _():
            up_in(s, k).wait_recv()

            @pl.when(hi)
            def _():
                up(s, k).start()

        @pl.when(c + s < C)
        def _():
            down_in(s, k).wait_recv()

            @pl.when(lo)
            def _():
                down(s, k).start()

    def phase(s, t_lo, t_hi, start, d_hi):
        def step(k, _):
            arrive(s, k)

            def each(t, _):
                i = c + (1 - 2 * (t % 2)) * ((t + 1) // 2)

                @pl.when((i >= 0) & (i < C))
                def _():
                    @pl.when(start(t) == 0)
                    def _():
                        panel(i, k)
                    compute(i, k, start(t), d_hi)
                return 0
            lax.fori_loop(t_lo, t_hi, each, 0)
            return 0
        lax.fori_loop(0, NC, step, 0)

    def own(k, _):
        panel(c, k)
        compute(c, k, 0, 1)
        return 0
    lax.fori_loop(0, NC, own, 0)

    for k in range(NC):
        arrive(1, k)
        for d in range(1, R - 1):
            gather(k, d).wait_recv()
        if relay:
            via = 1 if k < NC // 2 else 2
            forward(k, via, 3 - via).start()
    phase(2, 0, 3, lambda t: jnp.where(t == 0, 1, 0), R - 1)
    for k in range(NC):
        gather(k, R - 1).wait_recv()
    phase(3, 0, 7, lambda t: jnp.where(t < 3, R - 1, 0), R)
    if C > 4:
        def later(s, _):
            phase(s, 2 * s - 1, 2 * s + 1, lambda t: 0, R)
            return 0
        lax.fori_loop(4, C, later, 0)

    out_cp = []
    for d in range(1, R):
        q = pl.multiple_of(flip(r, d) * per, 8)
        for j in range(R):
            out_cp.append(rowcopy(macc.at[j, pl.ds(q, per), :], rs.at[d, j],
                                  s_rs.at[d, j], r_rs.at[d, j], d))
            out_cp[-1].start()
    for j in range(R):
        degb[j] = macc[j, W:W + 1, :]
    zs = zcol[r].astype(F32)
    self_term = power_eight(jnp.sum(zs * zs, axis=0, keepdims=True))
    degb[r] = degb[r] - self_term.astype(BF16).astype(F32)
    dg = []
    for d in range(1, R):
        dg.append(rowcopy(degb, degr.at[d], s_dg.at[d], r_dg.at[d], d))
        dg[-1].start()
    own_rows = pl.ds(pl.multiple_of(r * per, 8), per)
    for j in range(R):
        total = macc[j, own_rows, :]
        for d in range(1, R):
            out_cp[(d - 1) * R + j].wait_recv()
            total = total + rs[d, j]
        out[:, j * slab:(j + 1) * slab] = total
    for cp in dg:
        cp.wait_recv()
    for j in range(R):
        total = degb[j]
        for d in range(1, R):
            total = total + degr[d, j]
        dego[:, j * slab:(j + 1) * slab] = total

    for cp in st + aa + zc + zr + out_cp + dg:
        cp.wait_send()
    for k in range(NC):
        for d in range(1, R):
            gather(k, d).wait_send()

    def drain(s, _):
        def each(k, _):
            @pl.when(hi & (c - s >= 0))
            def _():
                up(s, k).wait_send()

            @pl.when(lo & (c + s < C))
            def _():
                down(s, k).wait_send()
            return 0
        lax.fori_loop(0, NC, each, 0)
        return 0
    lax.fori_loop(0, C - 1, drain, 0)


LIMIT = 65535.0


def quantize(v):
    h = v.shape[0] // 2
    top = jnp.maximum(jnp.max(v, axis=0, keepdims=True), 1e-20)
    inv = LIMIT / top
    code = (v * inv + 0.5).astype(jnp.int32)
    return code[:h] | lax.shift_left(code[h:], 16), top


def restore(code, top):
    unit = top * (1.0 / LIMIT)
    low = (code & 65535).astype(F32) * unit
    high = lax.shift_right_logical(code, 16).astype(F32) * unit
    return low, high


def gather_plan():
    plan = {}
    for d in (1, 2):
        e, sent, groups = d - 1, set(), []
        for m in range(4):
            group = []
            for piece in [(3 ^ m, e), (d ^ m, e), (d ^ m, 1 - e)]:
                if piece not in sent:
                    sent.add(piece)
                    group.append(piece)
            groups.append(group)
        plan[d] = groups
    return plan


def folded_kernel(eps, expr, win, out, dego,
                  stats, zcol, zf, zt, zw, zwr, zwt, zwn, pcol, prow, macc, ret,
                  rtq, rta, rbq, rba, rsq, rsa, rbufq, rbufa, degb, degr,
                  s_st, r_st, s_ag, r_ag, s_rl, s_z, r_z, s_zf, s_zc, r_zc, s_zr, r_zr,
                  s_rt, r_rt, s_rs, r_rs, s_dg, r_dg):
    R, C = 4, 4
    t = lax.axis_index("tissue")
    r = lax.axis_index("row")
    c = lax.axis_index("col")
    p = c + t * (C - 1 - 2 * c)
    S, width = expr.shape
    slab = width // R
    half = slab // 2
    pad = zcol.shape[1] // R
    W = zw.shape[2]
    per = W // R
    CH = zt.shape[1] // 2

    def rowpeer(d):
        return {"row": flip(r, d)}

    def colpeer(q):
        return {"col": q + t * (C - 1 - 2 * q)}

    def copy(src, dst, ss, rr, dev):
        return pltpu.make_async_remote_copy(
            src_ref=src, dst_ref=dst, send_sem=ss, recv_sem=rr,
            device_id=dev, device_id_type=MESH)

    started = []

    def send(src, dst, ss, rr, dev):
        cp = copy(src, dst, ss, rr, dev)
        cp.start()
        started.append(cp)

    def arrived(dst, rr):
        copy(dst, dst, rr, rr, rowpeer(1)).wait_recv()

    barrier = pltpu.get_barrier_semaphore()
    for d in range(1, R):
        pl.semaphore_signal(barrier, inc=1, device_id=rowpeer(d), device_id_type=MESH)
    for d in range(1, C):
        pl.semaphore_signal(barrier, inc=1, device_id={"col": lax.rem(c + d, C)}, device_id_type=MESH)

    def at(m):
        return pl.ds(pl.multiple_of(flip(r, m) * slab, 128), slab)

    for j in range(R):
        cols = slice(j * slab, (j + 1) * slab)
        x = expr[:, cols]
        total = jnp.sum(x, axis=0, keepdims=True)
        dev = x - total * (1.0 / S)
        stats[0, 0:1, cols] = total
        stats[0, 1:2, cols] = jnp.sum(dev * dev, axis=0, keepdims=True)
    pl.semaphore_wait(barrier, R + C - 2)
    for d in range(1, R):
        send(stats.at[0], stats.at[d], s_st.at[d], r_st.at[d], rowpeer(d))
    for m in range(R):
        zcol[m, pad - 16:pad, :] = jnp.zeros((16, slab), BF16)
        macc[m] = jnp.zeros(macc.shape[1:], F32)
        pcol[m, W:, :] = jnp.ones((16, slab), BF16)
    for f in range(2):
        prow[f, W:, :] = jnp.ones((16, slab), BF16)
        ret[f] = jnp.zeros(ret.shape[1:], F32)
    for d in range(1, R):
        arrived(stats.at[d], r_st.at[d])

    plan = gather_plan()

    def direct(d, g):
        for rel, e in plan[d][g]:
            cols = slice(e * half, (e + 1) * half)
            send(zcol.at[rel, 0:pad, cols], zcol.at[rel ^ d, d * pad:(d + 1) * pad, cols],
                 s_ag.at[d, rel, e], r_ag.at[d, rel ^ d, e], rowpeer(d))

    seen = set()

    def landed(d, m, e):
        if (d, m, e) in seen:
            return
        seen.add((d, m, e))
        cols = slice(e * half, (e + 1) * half)
        arrived(zcol.at[m, d * pad:(d + 1) * pad, cols], r_ag.at[d, m, e])

    def relay(g):
        for d in (1, 2):
            n, e = 3 - d, 2 - d
            rel = d ^ g
            cols = slice(e * half, (e + 1) * half)
            piece = zcol.at[rel, n * pad:(n + 1) * pad, cols]
            landed(n, rel, e)
            send(piece, zcol.at[g, 3 * pad:4 * pad, cols],
                 s_rl.at[d, g], r_ag.at[3, g, e], rowpeer(d))

    def gathered(m):
        for d in range(1, R):
            for e in range(2):
                landed(d, m, e)

    for m in (3, 1, 2, 0):
        cols = at(m)
        total = stats[0, 0:1, cols]
        for d in range(1, R):
            total = total + stats[d, 0:1, cols]
        mean = total / (S * R)
        sq = jnp.zeros_like(mean)
        for d in range(R):
            gap = stats[d, 0:1, cols] * (1.0 / S) - mean
            sq = sq + (stats[d, 1:2, cols] + S * gap * gap)
        inv = 1.0 / jnp.sqrt(sq + eps)
        zcol[m, 0:S, :] = ((expr[:, cols] - mean) * inv).astype(BF16)
        if m == 2:
            for d in (1, 2):
                direct(d, 0)

    zslot = p // 3
    zpeer = colpeer(jnp.where(p == 3, 1, p + 1))

    def zsend(d):
        rows = slice(d * pad, (d + 1) * pad)
        send(zcol.at[0, rows, :], zf.at[zslot, rows, :], s_z.at[d], r_z.at[zslot, d], zpeer)

    zsend(0)

    pick = jnp.zeros((pad, W), F32)
    for m in range(R):
        gene = lax.broadcasted_iota(jnp.int32, (slab, W), 0) + (c * width + flip(r, m) * slab)
        onehot = jnp.where(gene == win[...], 1.0, 0.0).astype(BF16)
        pick = pick + dot(zcol[m, 0:pad, :], onehot)
    zw[0] = pick.astype(BF16)
    for d in range(1, C):
        send(zw.at[0], zw.at[d], s_zc.at[d], r_zc.at[d], {"col": lax.rem(c + d, C)})

    relay(0)
    tot = zw[0].astype(F32)
    for d in range(1, C):
        arrived(zw.at[d], r_zc.at[d])
        tot = tot + zw[d].astype(F32)
    zwr[0] = tot.astype(BF16)
    for d in range(1, R):
        send(zwr.at[0], zwr.at[d], s_zr.at[d], r_zr.at[d], rowpeer(d))
    for d in (1, 2):
        direct(d, 1)
    for d in range(1, R):
        for e in range(2):
            landed(d, 0, e)
        zsend(d)

    zt[0] = zcol[0].T
    for d in range(1, R):
        arrived(zwr.at[d], r_zr.at[d])
    for d in range(R):
        zwt[d * pad:(d + 1) * pad, :] = zwr[d]
    zwn[...] = zwt[...].T

    def panel_col(m):
        pcol[m, 0:W, :] = power_eight(dot(zwn[...], zcol[m])).astype(BF16)

    def chunk(k):
        return pl.ds(pl.multiple_of(k * CH, 128), CH)

    def own(m):
        def step(k, _):
            rows = chunk(k)
            adj = power_eight(dot(zt[0, rows, :], zcol[m])).astype(BF16)
            macc[m] += dot(pcol[0, :, rows], adj)
            return 0
        lax.fori_loop(0, 2, step, 0)

    def cross(f, k, m):
        rows = chunk(k)
        adj = power_eight(dot(zt[1 + f, rows, :], zcol[m])).astype(BF16)
        macc[m] += dot(prow[f, :, rows], adj)
        ret[f, :, rows] += dot(pcol[m], adj, ((1,), (1,)))

    def crosses(f, m_lo, m_hi):
        def step(i, _):
            cross(f, lax.rem(i, 2), m_lo + i // 2)
            return 0
        lax.fori_loop(0, 2 * (m_hi - m_lo), step, 0)

    def prepare(f, known):
        for d in range(R):
            if d not in known:
                arrived(zf.at[f, d * pad:(d + 1) * pad, :], r_z.at[f, d])
        zt[1 + f] = zf[f].T
        prow[f, 0:W, :] = power_eight(dot(zwn[...], zf[f])).astype(BF16)

    def zcopy(f, d):
        rows = slice(d * pad, (d + 1) * pad)
        dest = 2 if f == 0 else 0
        return copy(zf.at[f, rows, :], zf.at[1, rows, :], s_zf.at[f, d], r_z.at[1, d], colpeer(dest))

    def zrelay(f, ds):
        @pl.when(p == 1)
        def _():
            for d in ds:
                arrived(zf.at[f, d * pad:(d + 1) * pad, :], r_z.at[f, d])
                zcopy(f, d).start()

    def retcopy(f, k):
        cols = slice(k * CH, (k + 1) * CH)
        if f == 0:
            dest, slot = p - 1, 0
        else:
            dest = jnp.where(p == 2, 0, 3)
            slot = (p + 1) // 2
        return [copy(rtq.at[f, :, cols], rbq.at[slot, :, cols], s_rt.at[f, k, 0], r_rt.at[slot, k, 0], colpeer(dest)),
                copy(rta.at[f, k], rba.at[slot, k], s_rt.at[f, k, 1], r_rt.at[slot, k, 1], colpeer(dest))]

    def give_back(f, k):
        cols = slice(k * CH, (k + 1) * CH)
        code, top = quantize(ret[f, 0:W, cols])
        rtq[f, :, cols] = code
        rta[f, k, 0:1, :] = top
        rta[f, k, 1:2, :] = ret[f, W:W + 1, cols]
        for cp in retcopy(f, k):
            cp.start()

    def take_back(slot):
        for k in range(2):
            cols = slice(k * CH, (k + 1) * CH)
            arrived(rbq.at[slot, :, cols], r_rt.at[slot, k, 0])
            arrived(rba.at[slot, k], r_rt.at[slot, k, 1])
            low, high = restore(rbq[slot, :, cols], rba[slot, k, 0:1, :])
            macc[0, 0:W // 2, cols] += low
            macc[0, W // 2:W, cols] += high
            macc[0, W:W + 1, cols] += rba[slot, k, 1:2, :]

    def scatter(m):
        for d in range(1, R):
            rows = pl.ds(pl.multiple_of(flip(r, d) * per, 8), per)
            code, top = quantize(macc[m, rows, :])
            rsq[d, m] = code
            rsa[d, m] = top
            send(rsq.at[d, m], rbufq.at[d, m ^ d], s_rs.at[d, m, 0], r_rs.at[d, m ^ d, 0], rowpeer(d))
            send(rsa.at[d, m], rbufa.at[d, m ^ d], s_rs.at[d, m, 1], r_rs.at[d, m ^ d, 1], rowpeer(d))

    early, late = p >= 1, p <= 2

    panel_col(0)
    own(0)
    relay(1)
    for d in (1, 2):
        direct(d, 2)
        direct(d, 3)
    zrelay(0, (0, 1))
    gathered(1)
    panel_col(1)
    own(1)
    relay(2)
    zrelay(0, (2, 3))
    zrelay(1, (0, 1))

    @pl.when(p == 1)
    def _():
        prepare(0, range(R))

    @pl.when(p >= 2)
    def _():
        prepare(0, ())

    @pl.when(early)
    def _():
        crosses(0, 0, 2)
    relay(3)
    gathered(2)
    panel_col(2)
    own(2)
    zrelay(1, (2, 3))

    @pl.when(early)
    def _():
        crosses(0, 2, 3)
    gathered(3)
    panel_col(3)
    own(3)

    @pl.when(early)
    def _():
        crosses(0, 3, 4)
        for k in range(2):
            give_back(0, k)

    @pl.when(p == 1)
    def _():
        prepare(1, range(R))

    @pl.when((p == 0) | (p == 2))
    def _():
        prepare(1, ())

    for k in range(2):
        @pl.when(late)
        def _():
            def step(m, _):
                cross(1, k, m)
                return 0
            lax.fori_loop(0, R, step, 0)
            give_back(1, k)
    for m in range(1, R):
        scatter(m)
    take_back(0)

    @pl.when((p == 0) | (p == 3))
    def _():
        take_back(1)

    zs = zcol[0].astype(F32)
    self_term = power_eight(jnp.sum(zs * zs, axis=0, keepdims=True))
    for m in range(R):
        degb[m] = macc[m, W:W + 1, :]
    degb[0] = degb[0] - self_term.astype(BF16).astype(F32)
    for d in range(1, R):
        send(degb, degr.at[d], s_dg.at[d], r_dg.at[d], rowpeer(d))
    scatter(0)

    hp = per // 2
    mine = pl.multiple_of(r * per, 8)
    for m in (1, 2, 3, 0):
        for q in range(2):
            acc = macc[m, pl.ds(mine + q * hp, hp), :]
            for d in range(1, R):
                if q == 0:
                    arrived(rbufq.at[d, m], r_rs.at[d, m, 0])
                    arrived(rbufa.at[d, m], r_rs.at[d, m, 1])
                acc = acc + restore(rbufq[d, m], rbufa[d, m])[q]
            out[q * hp:(q + 1) * hp, at(m)] = acc
    for d in range(1, R):
        arrived(degr.at[d], r_dg.at[d])
    for m in range(R):
        total = degb[m]
        for d in range(1, R):
            total = total + degr[d, m ^ d]
        dego[:, at(m)] = total

    for cp in started:
        cp.wait_send()

    @pl.when(p == 1)
    def _():
        for f in range(2):
            for d in range(R):
                zcopy(f, d).wait_send()

    @pl.when(early)
    def _():
        for k in range(2):
            for cp in retcopy(0, k):
                cp.wait_send()

    @pl.when(late)
    def _():
        for k in range(2):
            for cp in retcopy(1, k):
                cp.wait_send()


def folded(expr, win):
    R = C = 4
    S, width = expr.shape
    W = win.shape[0]
    pad = (S + 15) // 16 * 16
    slab = width // R
    V = pltpu.VMEM
    I32 = jnp.int32
    dma = pltpu.SemaphoreType.DMA
    vm = pl.BlockSpec(memory_space=pltpu.VMEM)
    half = slab // 2
    margin, degree = pl.pallas_call(
        functools.partial(folded_kernel, 1e-6),
        out_shape=(jax.ShapeDtypeStruct((W // R, width), F32),
                   jax.ShapeDtypeStruct((1, width), F32)),
        in_specs=[vm, vm],
        out_specs=(vm, vm),
        scratch_shapes=[
            V((R, 2, width), F32),
            V((R, R * pad, slab), BF16),
            V((2, R * pad, slab), BF16),
            V((3, slab, R * pad), BF16),
            V((C, pad, W), BF16),
            V((R, pad, W), BF16),
            V((R * pad, W), BF16),
            V((W, R * pad), BF16),
            V((R, W + 16, slab), BF16),
            V((2, W + 16, slab), BF16),
            V((R, W + 16, slab), F32),
            V((2, W + 16, slab), F32),
            V((2, W // 2, slab), I32),
            V((2, 2, 2, half), F32),
            V((2, W // 2, slab), I32),
            V((2, 2, 2, half), F32),
            V((R, R, W // R // 2, slab), I32),
            V((R, R, 1, slab), F32),
            V((R, R, W // R // 2, slab), I32),
            V((R, R, 1, slab), F32),
            V((R, 1, slab), F32),
            V((R, R, 1, slab), F32),
            dma((R,)), dma((R,)),
            dma((R, R, 2)), dma((R, R, 2)), dma((R, R)),
            dma((R,)), dma((2, R)), dma((2, R)),
            dma((C,)), dma((C,)), dma((R,)), dma((R,)),
            dma((2, 2, 2)), dma((2, 2, 2)),
            dma((R, R, 2)), dma((R, R, 2)),
            dma((R,)), dma((R,)),
        ],
        compiler_params=pltpu.CompilerParams(
            collective_id=0, has_side_effects=True, vmem_limit_bytes=60 << 20),
    )(expr, win.reshape(1, W))
    return margin, degree.reshape(width)


def solution(mesh):
    R, C = mesh.shape["row"], mesh.shape["col"]

    def body(expr, win):
        if R == 4 and C == 4:
            return folded(expr, win)
        S, width = expr.shape
        W = win.shape[0]
        pad = (S + 15) // 16 * 16
        slab = width // R
        chunk = min(256, slab)
        NC = slab // chunk
        V = pltpu.VMEM
        dma = pltpu.SemaphoreType.DMA
        vm = pl.BlockSpec(memory_space=pltpu.VMEM)
        margin, degree = pl.pallas_call(
            functools.partial(kernel, R, C, 1e-6),
            out_shape=(jax.ShapeDtypeStruct((W // R, width), F32),
                       jax.ShapeDtypeStruct((1, width), F32)),
            in_specs=[vm, vm],
            out_specs=(vm, vm),
            scratch_shapes=[
                V((R, 2, width), F32),
                V((pad, width), BF16),
                V((R, R * pad, slab), BF16),
                V((C, NC, chunk, R * pad), BF16),
                V((C, pad, W), BF16),
                V((R, pad, W), BF16),
                V((R * pad, W), BF16),
                V((C, NC, W + 16, chunk), BF16),
                V((R, W + 16, slab), F32),
                V((R, R, W // R, slab), F32),
                V((R, 1, slab), F32),
                V((R, R, 1, slab), F32),
                dma((R,)), dma((R,)), dma((NC, R)), dma((NC, R)), dma((NC, R)), dma((NC, R)),
                dma((C,)), dma((C,)), dma((R,)), dma((R,)),
                dma((C, NC)), dma((C, NC)), dma((C, NC)), dma((C, NC)),
                dma((R, R)), dma((R, R)), dma((R,)), dma((R,)),
            ],
            compiler_params=pltpu.CompilerParams(
                collective_id=0, has_side_effects=True, vmem_limit_bytes=56 << 20),
        )(expr, win.reshape(1, W))
        return margin, degree.reshape(width)

    in_specs = (P(("tissue", "row"), "col"), P())
    out_specs = (P(("tissue", "row"), "col"), P(("tissue", "col")))
    return jax.shard_map(body, mesh=mesh, in_specs=in_specs, out_specs=out_specs, check_vma=False)
```

```python
import functools

import jax
import jax.numpy as jnp
from jax import lax
from jax.experimental import pallas as pl
from jax.experimental.pallas import tpu as pltpu
from jax.sharding import PartitionSpec as P

MESH = pl.DeviceIdType.MESH
F32 = jnp.float32
BF16 = jnp.bfloat16


def power_eight(corr):
    half = (1.0 + corr) * 0.5
    half = half * half
    half = half * half
    return half * half


def flip(r, d):
    out = r
    for b in range(6):
        bit = 1 << b
        out = out + ((d // bit) % 2) * (1 - 2 * ((r // bit) % 2)) * bit
    return out


def dot(a, b, dims=((1,), (0,))):
    return lax.dot_general(a, b, (dims, ((), ())), preferred_element_type=F32)


def kernel(R, C, eps, expr, win, out, dego,
           stats, zl, zcol, zrt, zw, zwr, zwt, pbuf, macc, rs, degb, degr,
           s_st, r_st, s_aa, r_aa, s_ga, r_ga, s_zc, r_zc, s_zr, r_zr,
           s_up, r_up, s_dn, r_dn, s_rs, r_rs, s_dg, r_dg):
    r = lax.axis_index("row")
    c = lax.axis_index("col")
    S, width = expr.shape
    pad = zl.shape[0]
    slab = width // R
    W = zw.shape[2]
    per = W // R
    NC, chunk = zrt.shape[1], zrt.shape[2]

    barrier = pltpu.get_barrier_semaphore()
    for d in range(1, R):
        pl.semaphore_signal(barrier, inc=1, device_id={"row": flip(r, d)}, device_id_type=MESH)
    for d in range(1, C):
        pl.semaphore_signal(barrier, inc=1, device_id={"col": lax.rem(c + d, C)}, device_id_type=MESH)

    for j in range(R):
        cols = slice(j * slab, (j + 1) * slab)
        x = expr[:, cols]
        total = jnp.sum(x, axis=0, keepdims=True)
        dev = x - total * (1.0 / S)
        stats[0, 0:1, cols] = total
        stats[0, 1:2, cols] = jnp.sum(dev * dev, axis=0, keepdims=True)
    pl.semaphore_wait(barrier, R + C - 2)

    def rowcopy(src, dst, ss, rr, d):
        return pltpu.make_async_remote_copy(
            src_ref=src, dst_ref=dst, send_sem=ss, recv_sem=rr,
            device_id={"row": flip(r, d)}, device_id_type=MESH)

    def colcopy(src, dst, ss, rr, peer):
        return pltpu.make_async_remote_copy(
            src_ref=src, dst_ref=dst, send_sem=ss, recv_sem=rr,
            device_id={"col": peer}, device_id_type=MESH)

    st = [rowcopy(stats.at[0], stats.at[d], s_st.at[d], r_st.at[d], d) for d in range(1, R)]
    for cp in st:
        cp.start()
    macc[...] = jnp.zeros_like(macc)
    zl[pad - 16:pad, :] = jnp.zeros((16, width), BF16)
    pbuf[...] = jnp.ones_like(pbuf)
    for cp in st:
        cp.wait_recv()

    for j in range(R):
        cols = slice(j * slab, (j + 1) * slab)
        total = stats[0, 0:1, cols]
        for d in range(1, R):
            total = total + stats[d, 0:1, cols]
        mean = total / (S * R)
        sq = jnp.zeros_like(mean)
        for d in range(R):
            gap = stats[d, 0:1, cols] * (1.0 / S) - mean
            sq = sq + (stats[d, 1:2, cols] + S * gap * gap)
        inv = 1.0 / jnp.sqrt(sq + eps)
        zl[0:S, cols] = ((expr[:, cols] - mean) * inv).astype(BF16)

    mine = pl.ds(pl.multiple_of(r * pad, 16), pad)
    aa = []
    for k in range(NC):
        for d in range(1, R):
            q = flip(r, d)
            at = pl.multiple_of(q * slab + k * chunk, 128)
            aa.append(rowcopy(zl.at[:, pl.ds(at, chunk)],
                              zcol.at[q, mine, k * chunk:(k + 1) * chunk],
                              s_aa.at[k, d], r_aa.at[k, d], d))
            aa[-1].start()
    zcol[r, mine, :] = zl[:, pl.ds(pl.multiple_of(r * slab, 128), slab)]

    pick = jnp.zeros((pad, W), F32)
    for j in range(R):
        gene = lax.broadcasted_iota(jnp.int32, (slab, W), 0) + (c * width + j * slab)
        onehot = jnp.where(gene == win[...], 1.0, 0.0).astype(BF16)
        pick = pick + dot(zl[:, j * slab:(j + 1) * slab], onehot)
    zw[0] = pick.astype(BF16)
    zc = []
    for d in range(1, C):
        zc.append(colcopy(zw.at[0], zw.at[d], s_zc.at[d], r_zc.at[d], lax.rem(c + d, C)))
        zc[-1].start()

    zr_own = zcol.at[r]
    lo, hi = c > 0, c < C - 1

    def up(s, k):
        i = c - s
        return colcopy(zrt.at[i, k], zrt.at[i, k], s_up.at[s, k], r_up.at[s, k], c + 1)

    def up_in(s, k):
        i = c - s
        return colcopy(zrt.at[i, k], zrt.at[i, k], s_up.at[s - 1, k], r_up.at[s - 1, k], c + 1)

    def down(s, k):
        i = c + s
        return colcopy(zrt.at[i, k], zrt.at[i, k], s_dn.at[s, k], r_dn.at[s, k], c - 1)

    def down_in(s, k):
        i = c + s
        return colcopy(zrt.at[i, k], zrt.at[i, k], s_dn.at[s - 1, k], r_dn.at[s - 1, k], c - 1)

    for k in range(NC):
        for cp in aa[k * (R - 1):(k + 1) * (R - 1)]:
            cp.wait_recv()
        zrt[c, k] = zr_own[:, k * chunk:(k + 1) * chunk].T

        @pl.when(hi)
        def _():
            up(0, k).start()

        @pl.when(lo)
        def _():
            down(0, k).start()

    relay = R == 4

    def gather(k, d):
        piece = zcol.at[r, :, pl.ds(pl.multiple_of(k * chunk, 128), chunk)]
        return rowcopy(piece, piece, s_ga.at[k, d], r_ga.at[k, d], d)

    def forward(k, via, to):
        piece = zcol.at[flip(r, via), :, pl.ds(pl.multiple_of(k * chunk, 128), chunk)]
        return rowcopy(piece, piece, s_ga.at[k, R - 1], r_ga.at[k, R - 1], to)

    direct = R - 1 if relay else R
    for d in range(1, direct):
        gather(0, d).start()

    tot = zw[0].astype(F32)
    for cp in zc:
        cp.wait_recv()
    for d in range(1, C):
        tot = tot + zw[d].astype(F32)
    zwr[0] = tot.astype(BF16)
    zr = []
    for d in range(1, R):
        zr.append(rowcopy(zwr.at[0], zwr.at[d], s_zr.at[d], r_zr.at[d], d))
        zr[-1].start()
    for k in range(1, NC):
        for d in range(1, direct):
            gather(k, d).start()
    for cp in zr:
        cp.wait_recv()
    for d in range(R):
        zwt[pl.ds(pl.multiple_of(flip(r, d) * pad, 16), pad), :] = zwr[d]

    def compute(i, k, d_lo, d_hi):
        def one(d, _):
            j = flip(r, d)
            adj = power_eight(dot(zrt[i, k], zcol[j])).astype(BF16)
            macc[j] += dot(pbuf[i, k], adj)
            return 0
        lax.fori_loop(d_lo, d_hi, one, 0)

    def panel(i, k):
        pt = power_eight(dot(zrt[i, k], zwt[...])).T
        pbuf[i, k, 0:W, :] = pt.astype(BF16)

    def arrive(s, k):
        @pl.when(c - s >= 0)
        def _():
            up_in(s, k).wait_recv()

            @pl.when(hi)
            def _():
                up(s, k).start()

        @pl.when(c + s < C)
        def _():
            down_in(s, k).wait_recv()

            @pl.when(lo)
            def _():
                down(s, k).start()

    def phase(s, t_lo, t_hi, start, d_hi):
        def step(k, _):
            arrive(s, k)

            def each(t, _):
                i = c + (1 - 2 * (t % 2)) * ((t + 1) // 2)

                @pl.when((i >= 0) & (i < C))
                def _():
                    @pl.when(start(t) == 0)
                    def _():
                        panel(i, k)
                    compute(i, k, start(t), d_hi)
                return 0
            lax.fori_loop(t_lo, t_hi, each, 0)
            return 0
        lax.fori_loop(0, NC, step, 0)

    def own(k, _):
        panel(c, k)
        compute(c, k, 0, 1)
        return 0
    lax.fori_loop(0, NC, own, 0)

    for k in range(NC):
        arrive(1, k)
        for d in range(1, R - 1):
            gather(k, d).wait_recv()
        if relay:
            via = 1 if k < NC // 2 else 2
            forward(k, via, 3 - via).start()
    phase(2, 0, 3, lambda t: jnp.where(t == 0, 1, 0), R - 1)
    for k in range(NC):
        gather(k, R - 1).wait_recv()
    phase(3, 0, 7, lambda t: jnp.where(t < 3, R - 1, 0), R)
    if C > 4:
        def later(s, _):
            phase(s, 2 * s - 1, 2 * s + 1, lambda t: 0, R)
            return 0
        lax.fori_loop(4, C, later, 0)

    out_cp = []
    for d in range(1, R):
        q = pl.multiple_of(flip(r, d) * per, 8)
        for j in range(R):
            out_cp.append(rowcopy(macc.at[j, pl.ds(q, per), :], rs.at[d, j],
                                  s_rs.at[d, j], r_rs.at[d, j], d))
            out_cp[-1].start()
    for j in range(R):
        degb[j] = macc[j, W:W + 1, :]
    zs = zcol[r].astype(F32)
    self_term = power_eight(jnp.sum(zs * zs, axis=0, keepdims=True))
    degb[r] = degb[r] - self_term.astype(BF16).astype(F32)
    dg = []
    for d in range(1, R):
        dg.append(rowcopy(degb, degr.at[d], s_dg.at[d], r_dg.at[d], d))
        dg[-1].start()
    own_rows = pl.ds(pl.multiple_of(r * per, 8), per)
    for j in range(R):
        total = macc[j, own_rows, :]
        for d in range(1, R):
            out_cp[(d - 1) * R + j].wait_recv()
            total = total + rs[d, j]
        out[:, j * slab:(j + 1) * slab] = total
    for cp in dg:
        cp.wait_recv()
    for j in range(R):
        total = degb[j]
        for d in range(1, R):
            total = total + degr[d, j]
        dego[:, j * slab:(j + 1) * slab] = total

    for cp in st + aa + zc + zr + out_cp + dg:
        cp.wait_send()
    for k in range(NC):
        for d in range(1, R):
            gather(k, d).wait_send()

    def drain(s, _):
        def each(k, _):
            @pl.when(hi & (c - s >= 0))
            def _():
                up(s, k).wait_send()

            @pl.when(lo & (c + s < C))
            def _():
                down(s, k).wait_send()
            return 0
        lax.fori_loop(0, NC, each, 0)
        return 0
    lax.fori_loop(0, C - 1, drain, 0)


LIMIT = 65535.0


def quantize(v):
    h = v.shape[0] // 2
    top = jnp.maximum(jnp.max(v, axis=0, keepdims=True), 1e-20)
    inv = LIMIT / top
    code = (v * inv + 0.5).astype(jnp.int32)
    return code[:h] | lax.shift_left(code[h:], 16), top


def restore(code, top):
    unit = top * (1.0 / LIMIT)
    low = (code & 65535).astype(F32) * unit
    high = lax.shift_right_logical(code, 16).astype(F32) * unit
    return low, high


def gather_plan():
    plan = {}
    for d in (1, 2):
        e, sent, groups = d - 1, set(), []
        for m in range(4):
            group = []
            for piece in [(3 ^ m, e), (d ^ m, e), (d ^ m, 1 - e)]:
                if piece not in sent:
                    sent.add(piece)
                    group.append(piece)
            groups.append(group)
        plan[d] = groups
    return plan


def folded_kernel(eps, expr, win, out, dego,
                  stats, zcol, zf, zt, zw, zwr, zwt, zwn, pcol, prow, macc, ret,
                  rtq, rta, rbq, rba, rsq, rsa, rbufq, rbufa, degb, degr,
                  s_st, r_st, s_ag, r_ag, s_rl, s_z, r_z, s_zf, s_zc, r_zc, s_zr, r_zr,
                  s_rt, r_rt, s_rs, r_rs, s_dg, r_dg):
    R, C = 4, 4
    t = lax.axis_index("tissue")
    r = lax.axis_index("row")
    c = lax.axis_index("col")
    p = c + t * (C - 1 - 2 * c)
    S, width = expr.shape
    slab = width // R
    half = slab // 2
    pad = zcol.shape[1] // R
    W = zw.shape[2]
    per = W // R
    CH = zt.shape[1] // 2
    full = (S + 7) // 8 * 8

    def block(d):
        return slice(d * pad, d * pad + full)

    def rowpeer(d):
        return {"row": flip(r, d)}

    def colpeer(q):
        return {"col": q + t * (C - 1 - 2 * q)}

    def copy(src, dst, ss, rr, dev):
        return pltpu.make_async_remote_copy(
            src_ref=src, dst_ref=dst, send_sem=ss, recv_sem=rr,
            device_id=dev, device_id_type=MESH)

    started = []

    def send(src, dst, ss, rr, dev):
        cp = copy(src, dst, ss, rr, dev)
        cp.start()
        started.append(cp)

    def arrived(dst, rr):
        copy(dst, dst, rr, rr, rowpeer(1)).wait_recv()

    for d in range(R):
        tail = slice((d + 1) * pad - 16, (d + 1) * pad)
        for m in range(R):
            zcol[m, tail, :] = jnp.zeros((16, slab), BF16)
        for f in range(2):
            zf[f, tail, :] = jnp.zeros((16, slab), BF16)

    barrier = pltpu.get_barrier_semaphore()
    for d in range(1, R):
        pl.semaphore_signal(barrier, inc=1, device_id=rowpeer(d), device_id_type=MESH)
    for d in range(1, C):
        pl.semaphore_signal(barrier, inc=1, device_id={"col": lax.rem(c + d, C)}, device_id_type=MESH)

    def at(m):
        return pl.ds(pl.multiple_of(flip(r, m) * slab, 128), slab)

    for j in range(R):
        cols = slice(j * slab, (j + 1) * slab)
        x = expr[:, cols]
        total = jnp.sum(x, axis=0, keepdims=True)
        dev = x - total * (1.0 / S)
        stats[0, 0:1, cols] = total
        stats[0, 1:2, cols] = jnp.sum(dev * dev, axis=0, keepdims=True)
    pl.semaphore_wait(barrier, R + C - 2)
    for d in range(1, R):
        send(stats.at[0], stats.at[d], s_st.at[d], r_st.at[d], rowpeer(d))
    for m in range(R):
        macc[m] = jnp.zeros(macc.shape[1:], F32)
        pcol[m, W:, :] = jnp.ones((16, slab), BF16)
    for f in range(2):
        prow[f, W:, :] = jnp.ones((16, slab), BF16)
        ret[f] = jnp.zeros(ret.shape[1:], F32)
    for d in range(1, R):
        arrived(stats.at[d], r_st.at[d])

    plan = gather_plan()

    def direct(d, g):
        for rel, e in plan[d][g]:
            cols = slice(e * half, (e + 1) * half)
            send(zcol.at[rel, block(0), cols], zcol.at[rel ^ d, block(d), cols],
                 s_ag.at[d, rel, e], r_ag.at[d, rel ^ d, e], rowpeer(d))

    seen = set()

    def landed(d, m, e):
        if (d, m, e) in seen:
            return
        seen.add((d, m, e))
        cols = slice(e * half, (e + 1) * half)
        arrived(zcol.at[m, block(d), cols], r_ag.at[d, m, e])

    def relay(g, links=(1, 2)):
        for d in links:
            n, e = 3 - d, 2 - d
            rel = d ^ g
            cols = slice(e * half, (e + 1) * half)
            landed(n, rel, e)
            send(zcol.at[rel, block(n), cols], zcol.at[g, block(3), cols],
                 s_rl.at[d, g], r_ag.at[3, g, e], rowpeer(d))

    def gathered(m):
        for d in range(1, R):
            for e in range(2):
                landed(d, m, e)

    for m in (3, 1, 2, 0):
        cols = at(m)
        total = stats[0, 0:1, cols]
        for d in range(1, R):
            total = total + stats[d, 0:1, cols]
        mean = total / (S * R)
        sq = jnp.zeros_like(mean)
        for d in range(R):
            gap = stats[d, 0:1, cols] * (1.0 / S) - mean
            sq = sq + (stats[d, 1:2, cols] + S * gap * gap)
        inv = 1.0 / jnp.sqrt(sq + eps)
        zcol[m, 0:S, :] = ((expr[:, cols] - mean) * inv).astype(BF16)
        if m == 2:
            for d in (1, 2):
                direct(d, 0)

    zslot = p // 3
    zpeer = colpeer(jnp.where(p == 3, 1, p + 1))

    def zsend(d):
        rows = block(d)
        send(zcol.at[0, rows, :], zf.at[zslot, rows, :], s_z.at[d], r_z.at[zslot, d], zpeer)

    pick = jnp.zeros((pad, W), F32)
    for m in range(R):
        gene = lax.broadcasted_iota(jnp.int32, (slab, W), 0) + (c * width + flip(r, m) * slab)
        onehot = jnp.where(gene == win[...], 1.0, 0.0).astype(BF16)
        pick = pick + dot(zcol[m, 0:pad, :], onehot)
    zw[0] = pick.astype(BF16)
    for d in range(1, C):
        send(zw.at[0], zw.at[d], s_zc.at[d], r_zc.at[d], {"col": lax.rem(c + d, C)})
    zsend(0)

    relay(0)
    tot = zw[0].astype(F32)
    for d in range(1, C):
        arrived(zw.at[d], r_zc.at[d])
        tot = tot + zw[d].astype(F32)
    zwr[0] = tot.astype(BF16)
    for d in range(1, R):
        send(zwr.at[0], zwr.at[d], s_zr.at[d], r_zr.at[d], rowpeer(d))
    for d in (1, 2):
        direct(d, 1)
    for d in range(1, R):
        for e in range(2):
            landed(d, 0, e)
        zsend(d)

    zt[0] = zcol[0].T
    for d in range(1, R):
        arrived(zwr.at[d], r_zr.at[d])
    for d in range(R):
        zwt[d * pad:(d + 1) * pad, :] = zwr[d]
    zwn[...] = zwt[...].T

    def panel_col(m):
        pcol[m, 0:W, :] = power_eight(dot(zwn[...], zcol[m])).astype(BF16)

    def chunk(k):
        return pl.ds(pl.multiple_of(k * CH, 128), CH)

    def own(m):
        def step(k, _):
            rows = chunk(k)
            adj = power_eight(dot(zt[0, rows, :], zcol[m])).astype(BF16)
            macc[m] += dot(pcol[0, :, rows], adj)
            return 0
        lax.fori_loop(0, 2, step, 0)

    def cross(f, k, m):
        rows = chunk(k)
        adj = power_eight(dot(zt[1 + f, rows, :], zcol[m])).astype(BF16)
        macc[m] += dot(prow[f, :, rows], adj)
        ret[f, :, rows] += dot(pcol[m], adj, ((1,), (1,)))

    def crosses(f, m_lo, m_hi):
        def step(i, _):
            cross(f, lax.rem(i, 2), m_lo + i // 2)
            return 0
        lax.fori_loop(0, 2 * (m_hi - m_lo), step, 0)

    def prepare(f, known):
        for d in range(R):
            if d not in known:
                arrived(zf.at[f, block(d), :], r_z.at[f, d])
        zt[1 + f] = zf[f].T
        prow[f, 0:W, :] = power_eight(dot(zwn[...], zf[f])).astype(BF16)

    def zcopy(f, d):
        rows = block(d)
        dest = 2 if f == 0 else 0
        return copy(zf.at[f, rows, :], zf.at[1, rows, :], s_zf.at[f, d], r_z.at[1, d], colpeer(dest))

    def zrelay(f, ds):
        @pl.when(p == 1)
        def _():
            for d in ds:
                arrived(zf.at[f, block(d), :], r_z.at[f, d])
                zcopy(f, d).start()

    def back_copies(f, k):
        cols = slice(k * CH, (k + 1) * CH)
        if f == 0:
            dest, slot = p - 1, 0
        else:
            dest = jnp.where(p == 2, 0, 3)
            slot = (p + 1) // 2
        made = []
        for d in (3, 1, 2, 0):
            dev = {**colpeer(dest), **(rowpeer(d) if d else {})}
            made += [copy(rtq.at[f, d, :, cols], rbq.at[slot, d, :, cols],
                          s_rt.at[f, k, d, 0], r_rt.at[slot, k, d, 0], dev),
                     copy(rta.at[f, k, d], rba.at[slot, k, d],
                          s_rt.at[f, k, d, 1], r_rt.at[slot, k, d, 1], dev)]
        return made

    def give_back(f, k):
        cols = slice(k * CH, (k + 1) * CH)
        made = back_copies(f, k)
        for i, d in enumerate((3, 1, 2, 0)):
            rows = pl.ds(pl.multiple_of(flip(r, d) * per, 8), per)
            code, top = quantize(ret[f, rows, cols])
            rtq[f, d, :, cols] = code
            rta[f, k, d, 0:1, :] = top
            rta[f, k, d, 1:2, :] = ret[f, W:W + 1, cols]
            made[2 * i].start()
            made[2 * i + 1].start()

    def take_back(slot):
        for k in range(2):
            cols = slice(k * CH, (k + 1) * CH)
            for m in range(R):
                arrived(rbq.at[slot, m, :, cols], r_rt.at[slot, k, m, 0])
                arrived(rba.at[slot, k, m], r_rt.at[slot, k, m, 1])
                there = pl.ds(pl.multiple_of(flip(r, m) * slab + k * CH, 128), CH)
                low, high = restore(rbq[slot, m, :, cols], rba[slot, k, m, 0:1, :])
                out[0:hp, there] += low
                out[hp:per, there] += high
                dego[:, there] += rba[slot, k, m, 1:2, :]

    def scatter_copies(m):
        made = []
        for d in (3, 1, 2):
            made += [copy(rsq.at[d, m], rbufq.at[d, m ^ d], s_rs.at[d, m, 0], r_rs.at[d, m ^ d, 0], rowpeer(d)),
                     copy(rsa.at[d, m], rbufa.at[d, m ^ d], s_rs.at[d, m, 1], r_rs.at[d, m ^ d, 1], rowpeer(d))]
        return made

    def scatter(m):
        made = scatter_copies(m)
        for i, d in enumerate((3, 1, 2)):
            rows = pl.ds(pl.multiple_of(flip(r, d) * per, 8), per)
            code, top = quantize(macc[m, rows, :])
            rsq[d, m] = code
            rsa[d, m] = top
            made[2 * i].start()
            made[2 * i + 1].start()

    early, late = p >= 1, p <= 2
    mid = early & late
    hp = per // 2

    panel_col(0)
    own(0)
    relay(1)
    for d in (1, 2):
        direct(d, 2)
        direct(d, 3)
    zrelay(0, range(R))

    @pl.when(p == 1)
    def _():
        prepare(0, range(R))

    @pl.when(p >= 2)
    def _():
        prepare(0, ())

    @pl.when(early)
    def _():
        crosses(0, 0, 1)
    gathered(1)
    relay(2)
    panel_col(1)
    own(1)

    @pl.when(early)
    def _():
        cross(0, 0, 1)
    relay(3)
    zrelay(1, (0, 1))

    @pl.when(early)
    def _():
        cross(0, 1, 1)
    zrelay(1, (2, 3))

    @pl.when(p == 1)
    def _():
        prepare(1, range(R))

    @pl.when(p == 2)
    def _():
        prepare(1, ())

    @pl.when(mid)
    def _():
        crosses(1, 0, 2)

    @pl.when(early)
    def _():
        scatter(0)
        scatter(1)
    gathered(2)
    panel_col(2)
    gathered(3)
    panel_col(3)

    @pl.when(early)
    def _():
        for k in range(2):
            lax.fori_loop(2, R, lambda m, _: (cross(0, k, m), 0)[1], 0)
            give_back(0, k)

    @pl.when(mid)
    def _():
        for k in range(2):
            lax.fori_loop(2, R, lambda m, _: (cross(1, k, m), 0)[1], 0)
            give_back(1, k)
    lax.fori_loop(2, R, lambda m, _: (own(m), 0)[1], 0)

    @pl.when(early)
    def _():
        scatter(2)
        scatter(3)

    @pl.when(p == 0)
    def _():
        prepare(1, ())
        for m in range(R):
            crosses(1, m, m + 1)
            scatter(m)
        for k in range(2):
            give_back(1, k)

    zs = zcol[0].astype(F32)
    self_term = power_eight(jnp.sum(zs * zs, axis=0, keepdims=True))
    for m in range(R):
        degb[m] = macc[m, W:W + 1, :]
    degb[0] = degb[0] - self_term.astype(BF16).astype(F32)
    for d in range(1, R):
        send(degb, degr.at[d], s_dg.at[d], r_dg.at[d], rowpeer(d))

    mine = pl.multiple_of(r * per, 8)
    for m in range(R):
        for q in range(2):
            acc = macc[m, pl.ds(mine + q * hp, hp), :]
            for d in range(1, R):
                if q == 0:
                    arrived(rbufq.at[d, m], r_rs.at[d, m, 0])
                    arrived(rbufa.at[d, m], r_rs.at[d, m, 1])
                acc = acc + restore(rbufq[d, m], rbufa[d, m])[q]
            out[q * hp:(q + 1) * hp, at(m)] = acc
    for d in range(1, R):
        arrived(degr.at[d], r_dg.at[d])
    for m in range(R):
        total = degb[m]
        for d in range(1, R):
            total = total + degr[d, m ^ d]
        dego[:, at(m)] = total
    take_back(0)

    @pl.when((p == 0) | (p == 3))
    def _():
        take_back(1)

    for cp in started:
        cp.wait_send()
    for m in range(R):
        for cp in scatter_copies(m):
            cp.wait_send()

    @pl.when(p == 1)
    def _():
        for f in range(2):
            for d in range(R):
                zcopy(f, d).wait_send()

    @pl.when(early)
    def _():
        for k in range(2):
            for cp in back_copies(0, k):
                cp.wait_send()

    @pl.when(late)
    def _():
        for k in range(2):
            for cp in back_copies(1, k):
                cp.wait_send()


def folded(expr, win):
    R = C = 4
    S, width = expr.shape
    W = win.shape[0]
    pad = (S + 15) // 16 * 16
    slab = width // R
    V = pltpu.VMEM
    I32 = jnp.int32
    dma = pltpu.SemaphoreType.DMA
    vm = pl.BlockSpec(memory_space=pltpu.VMEM)
    half = slab // 2
    margin, degree = pl.pallas_call(
        functools.partial(folded_kernel, 1e-6),
        out_shape=(jax.ShapeDtypeStruct((W // R, width), F32),
                   jax.ShapeDtypeStruct((1, width), F32)),
        in_specs=[vm, vm],
        out_specs=(vm, vm),
        scratch_shapes=[
            V((R, 2, width), F32),
            V((R, R * pad, slab), BF16),
            V((2, R * pad, slab), BF16),
            V((3, slab, R * pad), BF16),
            V((C, pad, W), BF16),
            V((R, pad, W), BF16),
            V((R * pad, W), BF16),
            V((W, R * pad), BF16),
            V((R, W + 16, slab), BF16),
            V((2, W + 16, slab), BF16),
            V((R, W + 16, slab), F32),
            V((2, W + 16, slab), F32),
            V((2, R, W // R // 2, slab), I32),
            V((2, 2, R, 2, half), F32),
            V((2, R, W // R // 2, slab), I32),
            V((2, 2, R, 2, half), F32),
            V((R, R, W // R // 2, slab), I32),
            V((R, R, 1, slab), F32),
            V((R, R, W // R // 2, slab), I32),
            V((R, R, 1, slab), F32),
            V((R, 1, slab), F32),
            V((R, R, 1, slab), F32),
            dma((R,)), dma((R,)),
            dma((R, R, 2)), dma((R, R, 2)), dma((R, R)),
            dma((R,)), dma((2, R)), dma((2, R)),
            dma((C,)), dma((C,)), dma((R,)), dma((R,)),
            dma((2, 2, R, 2)), dma((2, 2, R, 2)),
            dma((R, R, 2)), dma((R, R, 2)),
            dma((R,)), dma((R,)),
        ],
        compiler_params=pltpu.CompilerParams(
            collective_id=0, has_side_effects=True, vmem_limit_bytes=60 << 20),
    )(expr, win.reshape(1, W))
    return margin, degree.reshape(width)


def solution(mesh):
    R, C = mesh.shape["row"], mesh.shape["col"]

    def body(expr, win):
        if R == 4 and C == 4:
            return folded(expr, win)
        S, width = expr.shape
        W = win.shape[0]
        pad = (S + 15) // 16 * 16
        slab = width // R
        chunk = min(256, slab)
        NC = slab // chunk
        V = pltpu.VMEM
        dma = pltpu.SemaphoreType.DMA
        vm = pl.BlockSpec(memory_space=pltpu.VMEM)
        margin, degree = pl.pallas_call(
            functools.partial(kernel, R, C, 1e-6),
            out_shape=(jax.ShapeDtypeStruct((W // R, width), F32),
                       jax.ShapeDtypeStruct((1, width), F32)),
            in_specs=[vm, vm],
            out_specs=(vm, vm),
            scratch_shapes=[
                V((R, 2, width), F32),
                V((pad, width), BF16),
                V((R, R * pad, slab), BF16),
                V((C, NC, chunk, R * pad), BF16),
                V((C, pad, W), BF16),
                V((R, pad, W), BF16),
                V((R * pad, W), BF16),
                V((C, NC, W + 16, chunk), BF16),
                V((R, W + 16, slab), F32),
                V((R, R, W // R, slab), F32),
                V((R, 1, slab), F32),
                V((R, R, 1, slab), F32),
                dma((R,)), dma((R,)), dma((NC, R)), dma((NC, R)), dma((NC, R)), dma((NC, R)),
                dma((C,)), dma((C,)), dma((R,)), dma((R,)),
                dma((C, NC)), dma((C, NC)), dma((C, NC)), dma((C, NC)),
                dma((R, R)), dma((R, R)), dma((R,)), dma((R,)),
            ],
            compiler_params=pltpu.CompilerParams(
                collective_id=0, has_side_effects=True, vmem_limit_bytes=56 << 20),
        )(expr, win.reshape(1, W))
        return margin, degree.reshape(width)

    in_specs = (P(("tissue", "row"), "col"), P())
    out_specs = (P(("tissue", "row"), "col"), P(("tissue", "col")))
    return jax.shard_map(body, mesh=mesh, in_specs=in_specs, out_specs=out_specs, check_vma=False)
```

```python
import functools

import jax
import jax.numpy as jnp
from jax import lax
from jax.experimental import pallas as pl
from jax.experimental.pallas import tpu as pltpu
from jax.sharding import PartitionSpec as P

MESH = pl.DeviceIdType.MESH
F32 = jnp.float32
BF16 = jnp.bfloat16


def power_eight(corr):
    half = (1.0 + corr) * 0.5
    half = half * half
    half = half * half
    return half * half


def flip(r, d):
    out = r
    for b in range(6):
        bit = 1 << b
        out = out + ((d // bit) % 2) * (1 - 2 * ((r // bit) % 2)) * bit
    return out


def dot(a, b, dims=((1,), (0,))):
    return lax.dot_general(a, b, (dims, ((), ())), preferred_element_type=F32)


def kernel(R, C, eps, expr, win, out, dego,
           stats, zl, zcol, zrt, zw, zwr, zwt, pbuf, macc, rs, degb, degr,
           s_st, r_st, s_aa, r_aa, s_ga, r_ga, s_zc, r_zc, s_zr, r_zr,
           s_up, r_up, s_dn, r_dn, s_rs, r_rs, s_dg, r_dg):
    r = lax.axis_index("row")
    c = lax.axis_index("col")
    S, width = expr.shape
    pad = zl.shape[0]
    slab = width // R
    W = zw.shape[2]
    per = W // R
    NC, chunk = zrt.shape[1], zrt.shape[2]

    barrier = pltpu.get_barrier_semaphore()
    for d in range(1, R):
        pl.semaphore_signal(barrier, inc=1, device_id={"row": flip(r, d)}, device_id_type=MESH)
    for d in range(1, C):
        pl.semaphore_signal(barrier, inc=1, device_id={"col": lax.rem(c + d, C)}, device_id_type=MESH)

    for j in range(R):
        cols = slice(j * slab, (j + 1) * slab)
        x = expr[:, cols]
        total = jnp.sum(x, axis=0, keepdims=True)
        dev = x - total * (1.0 / S)
        stats[0, 0:1, cols] = total
        stats[0, 1:2, cols] = jnp.sum(dev * dev, axis=0, keepdims=True)
    pl.semaphore_wait(barrier, R + C - 2)

    def rowcopy(src, dst, ss, rr, d):
        return pltpu.make_async_remote_copy(
            src_ref=src, dst_ref=dst, send_sem=ss, recv_sem=rr,
            device_id={"row": flip(r, d)}, device_id_type=MESH)

    def colcopy(src, dst, ss, rr, peer):
        return pltpu.make_async_remote_copy(
            src_ref=src, dst_ref=dst, send_sem=ss, recv_sem=rr,
            device_id={"col": peer}, device_id_type=MESH)

    st = [rowcopy(stats.at[0], stats.at[d], s_st.at[d], r_st.at[d], d) for d in range(1, R)]
    for cp in st:
        cp.start()
    macc[...] = jnp.zeros_like(macc)
    zl[pad - 16:pad, :] = jnp.zeros((16, width), BF16)
    pbuf[...] = jnp.ones_like(pbuf)
    for cp in st:
        cp.wait_recv()

    for j in range(R):
        cols = slice(j * slab, (j + 1) * slab)
        total = stats[0, 0:1, cols]
        for d in range(1, R):
            total = total + stats[d, 0:1, cols]
        mean = total / (S * R)
        sq = jnp.zeros_like(mean)
        for d in range(R):
            gap = stats[d, 0:1, cols] * (1.0 / S) - mean
            sq = sq + (stats[d, 1:2, cols] + S * gap * gap)
        inv = 1.0 / jnp.sqrt(sq + eps)
        zl[0:S, cols] = ((expr[:, cols] - mean) * inv).astype(BF16)

    mine = pl.ds(pl.multiple_of(r * pad, 16), pad)
    aa = []
    for k in range(NC):
        for d in range(1, R):
            q = flip(r, d)
            at = pl.multiple_of(q * slab + k * chunk, 128)
            aa.append(rowcopy(zl.at[:, pl.ds(at, chunk)],
                              zcol.at[q, mine, k * chunk:(k + 1) * chunk],
                              s_aa.at[k, d], r_aa.at[k, d], d))
            aa[-1].start()
    zcol[r, mine, :] = zl[:, pl.ds(pl.multiple_of(r * slab, 128), slab)]

    pick = jnp.zeros((pad, W), F32)
    for j in range(R):
        gene = lax.broadcasted_iota(jnp.int32, (slab, W), 0) + (c * width + j * slab)
        onehot = jnp.where(gene == win[...], 1.0, 0.0).astype(BF16)
        pick = pick + dot(zl[:, j * slab:(j + 1) * slab], onehot)
    zw[0] = pick.astype(BF16)
    zc = []
    for d in range(1, C):
        zc.append(colcopy(zw.at[0], zw.at[d], s_zc.at[d], r_zc.at[d], lax.rem(c + d, C)))
        zc[-1].start()

    zr_own = zcol.at[r]
    lo, hi = c > 0, c < C - 1

    def up(s, k):
        i = c - s
        return colcopy(zrt.at[i, k], zrt.at[i, k], s_up.at[s, k], r_up.at[s, k], c + 1)

    def up_in(s, k):
        i = c - s
        return colcopy(zrt.at[i, k], zrt.at[i, k], s_up.at[s - 1, k], r_up.at[s - 1, k], c + 1)

    def down(s, k):
        i = c + s
        return colcopy(zrt.at[i, k], zrt.at[i, k], s_dn.at[s, k], r_dn.at[s, k], c - 1)

    def down_in(s, k):
        i = c + s
        return colcopy(zrt.at[i, k], zrt.at[i, k], s_dn.at[s - 1, k], r_dn.at[s - 1, k], c - 1)

    for k in range(NC):
        for cp in aa[k * (R - 1):(k + 1) * (R - 1)]:
            cp.wait_recv()
        zrt[c, k] = zr_own[:, k * chunk:(k + 1) * chunk].T

        @pl.when(hi)
        def _():
            up(0, k).start()

        @pl.when(lo)
        def _():
            down(0, k).start()

    relay = R == 4

    def gather(k, d):
        piece = zcol.at[r, :, pl.ds(pl.multiple_of(k * chunk, 128), chunk)]
        return rowcopy(piece, piece, s_ga.at[k, d], r_ga.at[k, d], d)

    def forward(k, via, to):
        piece = zcol.at[flip(r, via), :, pl.ds(pl.multiple_of(k * chunk, 128), chunk)]
        return rowcopy(piece, piece, s_ga.at[k, R - 1], r_ga.at[k, R - 1], to)

    direct = R - 1 if relay else R
    for d in range(1, direct):
        gather(0, d).start()

    tot = zw[0].astype(F32)
    for cp in zc:
        cp.wait_recv()
    for d in range(1, C):
        tot = tot + zw[d].astype(F32)
    zwr[0] = tot.astype(BF16)
    zr = []
    for d in range(1, R):
        zr.append(rowcopy(zwr.at[0], zwr.at[d], s_zr.at[d], r_zr.at[d], d))
        zr[-1].start()
    for k in range(1, NC):
        for d in range(1, direct):
            gather(k, d).start()
    for cp in zr:
        cp.wait_recv()
    for d in range(R):
        zwt[pl.ds(pl.multiple_of(flip(r, d) * pad, 16), pad), :] = zwr[d]

    def compute(i, k, d_lo, d_hi):
        def one(d, _):
            j = flip(r, d)
            adj = power_eight(dot(zrt[i, k], zcol[j])).astype(BF16)
            macc[j] += dot(pbuf[i, k], adj)
            return 0
        lax.fori_loop(d_lo, d_hi, one, 0)

    def panel(i, k):
        pt = power_eight(dot(zrt[i, k], zwt[...])).T
        pbuf[i, k, 0:W, :] = pt.astype(BF16)

    def arrive(s, k):
        @pl.when(c - s >= 0)
        def _():
            up_in(s, k).wait_recv()

            @pl.when(hi)
            def _():
                up(s, k).start()

        @pl.when(c + s < C)
        def _():
            down_in(s, k).wait_recv()

            @pl.when(lo)
            def _():
                down(s, k).start()

    def phase(s, t_lo, t_hi, start, d_hi):
        def step(k, _):
            arrive(s, k)

            def each(t, _):
                i = c + (1 - 2 * (t % 2)) * ((t + 1) // 2)

                @pl.when((i >= 0) & (i < C))
                def _():
                    @pl.when(start(t) == 0)
                    def _():
                        panel(i, k)
                    compute(i, k, start(t), d_hi)
                return 0
            lax.fori_loop(t_lo, t_hi, each, 0)
            return 0
        lax.fori_loop(0, NC, step, 0)

    def own(k, _):
        panel(c, k)
        compute(c, k, 0, 1)
        return 0
    lax.fori_loop(0, NC, own, 0)

    for k in range(NC):
        arrive(1, k)
        for d in range(1, R - 1):
            gather(k, d).wait_recv()
        if relay:
            via = 1 if k < NC // 2 else 2
            forward(k, via, 3 - via).start()
    phase(2, 0, 3, lambda t: jnp.where(t == 0, 1, 0), R - 1)
    for k in range(NC):
        gather(k, R - 1).wait_recv()
    phase(3, 0, 7, lambda t: jnp.where(t < 3, R - 1, 0), R)
    if C > 4:
        def later(s, _):
            phase(s, 2 * s - 1, 2 * s + 1, lambda t: 0, R)
            return 0
        lax.fori_loop(4, C, later, 0)

    out_cp = []
    for d in range(1, R):
        q = pl.multiple_of(flip(r, d) * per, 8)
        for j in range(R):
            out_cp.append(rowcopy(macc.at[j, pl.ds(q, per), :], rs.at[d, j],
                                  s_rs.at[d, j], r_rs.at[d, j], d))
            out_cp[-1].start()
    for j in range(R):
        degb[j] = macc[j, W:W + 1, :]
    zs = zcol[r].astype(F32)
    self_term = power_eight(jnp.sum(zs * zs, axis=0, keepdims=True))
    degb[r] = degb[r] - self_term.astype(BF16).astype(F32)
    dg = []
    for d in range(1, R):
        dg.append(rowcopy(degb, degr.at[d], s_dg.at[d], r_dg.at[d], d))
        dg[-1].start()
    own_rows = pl.ds(pl.multiple_of(r * per, 8), per)
    for j in range(R):
        total = macc[j, own_rows, :]
        for d in range(1, R):
            out_cp[(d - 1) * R + j].wait_recv()
            total = total + rs[d, j]
        out[:, j * slab:(j + 1) * slab] = total
    for cp in dg:
        cp.wait_recv()
    for j in range(R):
        total = degb[j]
        for d in range(1, R):
            total = total + degr[d, j]
        dego[:, j * slab:(j + 1) * slab] = total

    for cp in st + aa + zc + zr + out_cp + dg:
        cp.wait_send()
    for k in range(NC):
        for d in range(1, R):
            gather(k, d).wait_send()

    def drain(s, _):
        def each(k, _):
            @pl.when(hi & (c - s >= 0))
            def _():
                up(s, k).wait_send()

            @pl.when(lo & (c + s < C))
            def _():
                down(s, k).wait_send()
            return 0
        lax.fori_loop(0, NC, each, 0)
        return 0
    lax.fori_loop(0, C - 1, drain, 0)


LIMIT = 65535.0


def quantize(v):
    h = v.shape[0] // 2
    top = jnp.maximum(jnp.max(v, axis=0, keepdims=True), 1e-20)
    inv = LIMIT / top
    code = (v * inv + 0.5).astype(jnp.int32)
    return code[:h] | lax.shift_left(code[h:], 16), top


def restore(code, top):
    unit = top * (1.0 / LIMIT)
    low = (code & 65535).astype(F32) * unit
    high = lax.shift_right_logical(code, 16).astype(F32) * unit
    return low, high


def gather_plan():
    plan = {}
    for d in (1, 2):
        e, sent, groups = d - 1, set(), []
        for m in range(4):
            group = []
            for piece in [(3 ^ m, e), (d ^ m, e), (d ^ m, 1 - e)]:
                if piece not in sent:
                    sent.add(piece)
                    group.append(piece)
            groups.append(group)
        plan[d] = groups
    return plan


def folded_kernel(eps, expr, win, out, dego,
                  stats, zcol, zf, zt, zw, zwr, zwt, zwn, pcol, prow, macc, ret,
                  rtq, rta, rbq, rba, rsq, rsa, rbufq, rbufa, degb, degr,
                  s_st, r_st, s_ag, r_ag, s_rl, s_z, r_z, s_zf, s_zc, r_zc, s_zr, r_zr,
                  s_rt, r_rt, s_rs, r_rs, s_dg, r_dg):
    R, C = 4, 4
    t = lax.axis_index("tissue")
    r = lax.axis_index("row")
    c = lax.axis_index("col")
    p = c + t * (C - 1 - 2 * c)
    S, width = expr.shape
    slab = width // R
    half = slab // 2
    pad = zcol.shape[1] // R
    W = zw.shape[2]
    per = W // R
    CH = zt.shape[1] // 2
    full = (S + 7) // 8 * 8

    def block(d):
        return slice(d * pad, d * pad + full)

    def rowpeer(d):
        return {"row": flip(r, d)}

    def colpeer(q):
        return {"col": q + t * (C - 1 - 2 * q)}

    def copy(src, dst, ss, rr, dev):
        return pltpu.make_async_remote_copy(
            src_ref=src, dst_ref=dst, send_sem=ss, recv_sem=rr,
            device_id=dev, device_id_type=MESH)

    started = []

    def send(src, dst, ss, rr, dev):
        cp = copy(src, dst, ss, rr, dev)
        cp.start()
        started.append(cp)

    def arrived(dst, rr):
        copy(dst, dst, rr, rr, rowpeer(1)).wait_recv()

    for d in range(R):
        tail = slice((d + 1) * pad - 16, (d + 1) * pad)
        for m in range(R):
            zcol[m, tail, :] = jnp.zeros((16, slab), BF16)
        for f in range(2):
            zf[f, tail, :] = jnp.zeros((16, slab), BF16)

    barrier = pltpu.get_barrier_semaphore()
    for d in range(1, R):
        pl.semaphore_signal(barrier, inc=1, device_id=rowpeer(d), device_id_type=MESH)
    for d in range(1, C):
        pl.semaphore_signal(barrier, inc=1, device_id={"col": lax.rem(c + d, C)}, device_id_type=MESH)

    def at(m):
        return pl.ds(pl.multiple_of(flip(r, m) * slab, 128), slab)

    for j in range(R):
        cols = slice(j * slab, (j + 1) * slab)
        x = expr[:, cols]
        total = jnp.sum(x, axis=0, keepdims=True)
        dev = x - total * (1.0 / S)
        stats[0, 0:1, cols] = total
        stats[0, 1:2, cols] = jnp.sum(dev * dev, axis=0, keepdims=True)
    pl.semaphore_wait(barrier, R + C - 2)
    for d in range(1, R):
        send(stats.at[0], stats.at[d], s_st.at[d], r_st.at[d], rowpeer(d))
    for m in range(R):
        macc[m] = jnp.zeros(macc.shape[1:], F32)
        pcol[m, W:, :] = jnp.ones((16, slab), BF16)
    for f in range(2):
        prow[f, W:, :] = jnp.ones((16, slab), BF16)
        ret[f] = jnp.zeros(ret.shape[1:], F32)
    for d in range(1, R):
        arrived(stats.at[d], r_st.at[d])

    plan = gather_plan()

    def direct(d, g):
        for rel, e in plan[d][g]:
            cols = slice(e * half, (e + 1) * half)
            send(zcol.at[rel, block(0), cols], zcol.at[rel ^ d, block(d), cols],
                 s_ag.at[d, rel, e], r_ag.at[d, rel ^ d, e], rowpeer(d))

    seen = set()

    def landed(d, m, e):
        if (d, m, e) in seen:
            return
        seen.add((d, m, e))
        cols = slice(e * half, (e + 1) * half)
        arrived(zcol.at[m, block(d), cols], r_ag.at[d, m, e])

    def relay(g, links=(1, 2)):
        for d in links:
            n, e = 3 - d, 2 - d
            rel = d ^ g
            cols = slice(e * half, (e + 1) * half)
            landed(n, rel, e)
            send(zcol.at[rel, block(n), cols], zcol.at[g, block(3), cols],
                 s_rl.at[d, g], r_ag.at[3, g, e], rowpeer(d))

    def gathered(m):
        for d in range(1, R):
            for e in range(2):
                landed(d, m, e)

    for m in (3, 1, 2, 0):
        cols = at(m)
        total = stats[0, 0:1, cols]
        for d in range(1, R):
            total = total + stats[d, 0:1, cols]
        mean = total / (S * R)
        sq = jnp.zeros_like(mean)
        for d in range(R):
            gap = stats[d, 0:1, cols] * (1.0 / S) - mean
            sq = sq + (stats[d, 1:2, cols] + S * gap * gap)
        inv = 1.0 / jnp.sqrt(sq + eps)
        zcol[m, 0:S, :] = ((expr[:, cols] - mean) * inv).astype(BF16)
        if m == 2:
            for d in (1, 2):
                direct(d, 0)

    zslot = p // 3
    zpeer = colpeer(jnp.where(p == 3, 1, p + 1))

    def zsend_copy(d):
        rows = block(d)
        return copy(zcol.at[0, rows, :], zf.at[zslot, rows, :], s_z.at[d], r_z.at[zslot, d], zpeer)

    def zsend(ds, cond):
        @pl.when(cond)
        def _():
            for d in ds:
                zsend_copy(d).start()

    pick = jnp.zeros((pad, W), F32)
    for m in range(R):
        gene = lax.broadcasted_iota(jnp.int32, (slab, W), 0) + (c * width + flip(r, m) * slab)
        onehot = jnp.where(gene == win[...], 1.0, 0.0).astype(BF16)
        pick = pick + dot(zcol[m, 0:pad, :], onehot)
    zw[0] = pick.astype(BF16)
    for d in range(1, C):
        send(zw.at[0], zw.at[d], s_zc.at[d], r_zc.at[d], {"col": lax.rem(c + d, C)})
    zsend((0,), p >= 0)

    relay(0)
    tot = zw[0].astype(F32)
    for d in range(1, C):
        arrived(zw.at[d], r_zc.at[d])
        tot = tot + zw[d].astype(F32)
    zwr[0] = tot.astype(BF16)
    for d in range(1, R):
        send(zwr.at[0], zwr.at[d], s_zr.at[d], r_zr.at[d], rowpeer(d))
    for d in (1, 2):
        direct(d, 1)
    for d in range(1, R):
        for e in range(2):
            landed(d, 0, e)
        zsend((d,), p < 3)

    zt[0] = zcol[0].T
    for d in range(1, R):
        arrived(zwr.at[d], r_zr.at[d])
    for d in range(R):
        zwt[d * pad:(d + 1) * pad, :] = zwr[d]
    zwn[...] = zwt[...].T

    def panel_col(m):
        pcol[m, 0:W, :] = power_eight(dot(zwn[...], zcol[m])).astype(BF16)

    def chunk(k):
        return pl.ds(pl.multiple_of(k * CH, 128), CH)

    def own(m):
        def step(k, _):
            rows = chunk(k)
            adj = power_eight(dot(zt[0, rows, :], zcol[m])).astype(BF16)
            macc[m] += dot(pcol[0, :, rows], adj)
            return 0
        lax.fori_loop(0, 2, step, 0)

    def cross(f, k, m):
        rows = chunk(k)
        adj = power_eight(dot(zt[1 + f, rows, :], zcol[m])).astype(BF16)
        macc[m] += dot(prow[f, :, rows], adj)
        ret[f, :, rows] += dot(pcol[m], adj, ((1,), (1,)))

    def crosses(f, m_lo, m_hi):
        def step(i, _):
            cross(f, lax.rem(i, 2), m_lo + i // 2)
            return 0
        lax.fori_loop(0, 2 * (m_hi - m_lo), step, 0)

    def prepare(f):
        zt[1 + f] = zf[f].T
        prow[f, 0:W, :] = power_eight(dot(zwn[...], zf[f])).astype(BF16)

    def zwait(f, ds):
        for d in ds:
            arrived(zf.at[f, block(d), :], r_z.at[f, d])

    def zrelay_copy(f, d):
        rows = block(d)
        return copy(zf.at[f, rows, :], zf.at[1, rows, :], s_zf.at[f, d], r_z.at[1, d], colpeer(2 + f))

    def zrelay(f, ds):
        @pl.when(p == 1 + f)
        def _():
            for d in ds:
                zwait(f, (d,))
                zrelay_copy(f, d).start()

    def back_copies(f, k):
        cols = slice(k * CH, (k + 1) * CH)
        if f == 0:
            dest, slot = p - 1, 0
        else:
            dest, slot = jnp.where(p == 1, 3, 0), p - 1
        made = []
        for d in (3, 1, 2, 0):
            dev = {**colpeer(dest), **(rowpeer(d) if d else {})}
            made += [copy(rtq.at[f, d, :, cols], rbq.at[slot, d, :, cols],
                          s_rt.at[f, k, d, 0], r_rt.at[slot, k, d, 0], dev),
                     copy(rta.at[f, k, d], rba.at[slot, k, d],
                          s_rt.at[f, k, d, 1], r_rt.at[slot, k, d, 1], dev)]
        return made

    def give_back(f, k):
        cols = slice(k * CH, (k + 1) * CH)
        made = back_copies(f, k)
        for i, d in enumerate((3, 1, 2, 0)):
            rows = pl.ds(pl.multiple_of(flip(r, d) * per, 8), per)
            code, top = quantize(ret[f, rows, cols])
            rtq[f, d, :, cols] = code
            rta[f, k, d, 0:1, :] = top
            rta[f, k, d, 1:2, :] = ret[f, W:W + 1, cols]
            made[2 * i].start()
            made[2 * i + 1].start()

    def take_back(slot):
        for k in range(2):
            cols = slice(k * CH, (k + 1) * CH)
            for m in range(R):
                arrived(rbq.at[slot, m, :, cols], r_rt.at[slot, k, m, 0])
                arrived(rba.at[slot, k, m], r_rt.at[slot, k, m, 1])
                there = pl.ds(pl.multiple_of(flip(r, m) * slab + k * CH, 128), CH)
                low, high = restore(rbq[slot, m, :, cols], rba[slot, k, m, 0:1, :])
                out[0:hp, there] += low
                out[hp:per, there] += high
                dego[:, there] += rba[slot, k, m, 1:2, :]

    def scatter_copies(m):
        made = []
        for d in (3, 1, 2):
            made += [copy(rsq.at[d, m], rbufq.at[d, m ^ d], s_rs.at[d, m, 0], r_rs.at[d, m ^ d, 0], rowpeer(d)),
                     copy(rsa.at[d, m], rbufa.at[d, m ^ d], s_rs.at[d, m, 1], r_rs.at[d, m ^ d, 1], rowpeer(d))]
        return made

    def scatter(m):
        made = scatter_copies(m)
        for i, d in enumerate((3, 1, 2)):
            rows = pl.ds(pl.multiple_of(flip(r, d) * per, 8), per)
            code, top = quantize(macc[m, rows, :])
            rsq[d, m] = code
            rsa[d, m] = top
            made[2 * i].start()
            made[2 * i + 1].start()

    away = p >= 1
    hp = per // 2

    panel_col(0)
    own(0)
    relay(1)
    for d in (1, 2):
        direct(d, 2)
        direct(d, 3)
    zrelay(0, range(R))

    @pl.when(p >= 2)
    def _():
        zwait(0, range(R))

    @pl.when(away)
    def _():
        prepare(0)
        crosses(0, 0, 1)
    gathered(1)
    relay(2)
    panel_col(1)
    own(1)
    relay(3)
    zsend((1, 2, 3), p == 3)
    zrelay(1, (0,))

    @pl.when(away)
    def _():
        crosses(0, 1, 2)
    zrelay(1, (1, 2))
    gathered(2)
    panel_col(2)
    gathered(3)
    panel_col(3)
    for k in range(2):
        @pl.when(away)
        def _():
            lax.fori_loop(2, R, lambda m, _: (cross(0, k, m), 0)[1], 0)
            give_back(0, k)
        if k == 0:
            zrelay(1, (3,))

    @pl.when((p == 1) | (p == 3))
    def _():
        zwait(1, range(R))

    @pl.when(away)
    def _():
        prepare(1)
    for m in range(2):
        @pl.when(away)
        def _():
            crosses(1, m, m + 1)
        scatter(m)

    @pl.when(away)
    def _():
        for k in range(2):
            lax.fori_loop(2, R, lambda m, _: (cross(1, k, m), 0)[1], 0)
            give_back(1, k)
    for m in range(2, R):
        own(m)
        scatter(m)

    zs = zcol[0].astype(F32)
    self_term = power_eight(jnp.sum(zs * zs, axis=0, keepdims=True))
    for m in range(R):
        degb[m] = macc[m, W:W + 1, :]
    degb[0] = degb[0] - self_term.astype(BF16).astype(F32)
    for d in range(1, R):
        send(degb, degr.at[d], s_dg.at[d], r_dg.at[d], rowpeer(d))

    mine = pl.multiple_of(r * per, 8)
    for m in range(R):
        for q in range(2):
            acc = macc[m, pl.ds(mine + q * hp, hp), :]
            for d in range(1, R):
                if q == 0:
                    arrived(rbufq.at[d, m], r_rs.at[d, m, 0])
                    arrived(rbufa.at[d, m], r_rs.at[d, m, 1])
                acc = acc + restore(rbufq[d, m], rbufa[d, m])[q]
            out[q * hp:(q + 1) * hp, at(m)] = acc
    for d in range(1, R):
        arrived(degr.at[d], r_dg.at[d])
    for m in range(R):
        total = degb[m]
        for d in range(1, R):
            total = total + degr[d, m ^ d]
        dego[:, at(m)] = total
    take_back(0)

    @pl.when(p == 0)
    def _():
        take_back(1)
        take_back(2)

    for cp in started:
        cp.wait_send()
    for m in range(R):
        for cp in scatter_copies(m):
            cp.wait_send()

    for d in range(R):
        zsend_copy(d).wait_send()

    for f in range(2):
        @pl.when(p == 1 + f)
        def _():
            for d in range(R):
                zrelay_copy(f, d).wait_send()

    @pl.when(away)
    def _():
        for f in range(2):
            for k in range(2):
                for cp in back_copies(f, k):
                    cp.wait_send()


def folded(expr, win):
    R = C = 4
    S, width = expr.shape
    W = win.shape[0]
    pad = (S + 15) // 16 * 16
    slab = width // R
    V = pltpu.VMEM
    I32 = jnp.int32
    dma = pltpu.SemaphoreType.DMA
    vm = pl.BlockSpec(memory_space=pltpu.VMEM)
    half = slab // 2
    margin, degree = pl.pallas_call(
        functools.partial(folded_kernel, 1e-6),
        out_shape=(jax.ShapeDtypeStruct((W // R, width), F32),
                   jax.ShapeDtypeStruct((1, width), F32)),
        in_specs=[vm, vm],
        out_specs=(vm, vm),
        scratch_shapes=[
            V((R, 2, width), F32),
            V((R, R * pad, slab), BF16),
            V((2, R * pad, slab), BF16),
            V((3, slab, R * pad), BF16),
            V((C, pad, W), BF16),
            V((R, pad, W), BF16),
            V((R * pad, W), BF16),
            V((W, R * pad), BF16),
            V((R, W + 16, slab), BF16),
            V((2, W + 16, slab), BF16),
            V((R, W + 16, slab), F32),
            V((2, W + 16, slab), F32),
            V((2, R, W // R // 2, slab), I32),
            V((2, 2, R, 2, half), F32),
            V((3, R, W // R // 2, slab), I32),
            V((3, 2, R, 2, half), F32),
            V((R, R, W // R // 2, slab), I32),
            V((R, R, 1, slab), F32),
            V((R, R, W // R // 2, slab), I32),
            V((R, R, 1, slab), F32),
            V((R, 1, slab), F32),
            V((R, R, 1, slab), F32),
            dma((R,)), dma((R,)),
            dma((R, R, 2)), dma((R, R, 2)), dma((R, R)),
            dma((R,)), dma((2, R)), dma((2, R)),
            dma((C,)), dma((C,)), dma((R,)), dma((R,)),
            dma((2, 2, R, 2)), dma((3, 2, R, 2)),
            dma((R, R, 2)), dma((R, R, 2)),
            dma((R,)), dma((R,)),
        ],
        compiler_params=pltpu.CompilerParams(
            collective_id=0, has_side_effects=True, vmem_limit_bytes=46 << 20),
    )(expr, win.reshape(1, W))
    return margin, degree.reshape(width)


def solution(mesh):
    R, C = mesh.shape["row"], mesh.shape["col"]

    def body(expr, win):
        if R == 4 and C == 4:
            return folded(expr, win)
        S, width = expr.shape
        W = win.shape[0]
        pad = (S + 15) // 16 * 16
        slab = width // R
        chunk = min(256, slab)
        NC = slab // chunk
        V = pltpu.VMEM
        dma = pltpu.SemaphoreType.DMA
        vm = pl.BlockSpec(memory_space=pltpu.VMEM)
        margin, degree = pl.pallas_call(
            functools.partial(kernel, R, C, 1e-6),
            out_shape=(jax.ShapeDtypeStruct((W // R, width), F32),
                       jax.ShapeDtypeStruct((1, width), F32)),
            in_specs=[vm, vm],
            out_specs=(vm, vm),
            scratch_shapes=[
                V((R, 2, width), F32),
                V((pad, width), BF16),
                V((R, R * pad, slab), BF16),
                V((C, NC, chunk, R * pad), BF16),
                V((C, pad, W), BF16),
                V((R, pad, W), BF16),
                V((R * pad, W), BF16),
                V((C, NC, W + 16, chunk), BF16),
                V((R, W + 16, slab), F32),
                V((R, R, W // R, slab), F32),
                V((R, 1, slab), F32),
                V((R, R, 1, slab), F32),
                dma((R,)), dma((R,)), dma((NC, R)), dma((NC, R)), dma((NC, R)), dma((NC, R)),
                dma((C,)), dma((C,)), dma((R,)), dma((R,)),
                dma((C, NC)), dma((C, NC)), dma((C, NC)), dma((C, NC)),
                dma((R, R)), dma((R, R)), dma((R,)), dma((R,)),
            ],
            compiler_params=pltpu.CompilerParams(
                collective_id=0, has_side_effects=True, vmem_limit_bytes=56 << 20),
        )(expr, win.reshape(1, W))
        return margin, degree.reshape(width)

    in_specs = (P(("tissue", "row"), "col"), P())
    out_specs = (P(("tissue", "row"), "col"), P(("tissue", "col")))
    return jax.shard_map(body, mesh=mesh, in_specs=in_specs, out_specs=out_specs, check_vma=False)
```

```python
import functools

import jax
import jax.numpy as jnp
from jax import lax
from jax.experimental import pallas as pl
from jax.experimental.pallas import tpu as pltpu
from jax.sharding import PartitionSpec as P

MESH = pl.DeviceIdType.MESH
F32 = jnp.float32
BF16 = jnp.bfloat16


def power_eight(corr):
    half = (1.0 + corr) * 0.5
    half = half * half
    half = half * half
    return half * half


def flip(r, d):
    out = r
    for b in range(6):
        bit = 1 << b
        out = out + ((d // bit) % 2) * (1 - 2 * ((r // bit) % 2)) * bit
    return out


def dot(a, b, dims=((1,), (0,))):
    return lax.dot_general(a, b, (dims, ((), ())), preferred_element_type=F32)


def kernel(R, C, eps, expr, win, out, dego,
           stats, zl, zcol, zrt, zw, zwr, zwt, pbuf, macc, rs, degb, degr,
           s_st, r_st, s_aa, r_aa, s_ga, r_ga, s_zc, r_zc, s_zr, r_zr,
           s_up, r_up, s_dn, r_dn, s_rs, r_rs, s_dg, r_dg):
    r = lax.axis_index("row")
    c = lax.axis_index("col")
    S, width = expr.shape
    pad = zl.shape[0]
    slab = width // R
    W = zw.shape[2]
    per = W // R
    NC, chunk = zrt.shape[1], zrt.shape[2]

    barrier = pltpu.get_barrier_semaphore()
    for d in range(1, R):
        pl.semaphore_signal(barrier, inc=1, device_id={"row": flip(r, d)}, device_id_type=MESH)
    for d in range(1, C):
        pl.semaphore_signal(barrier, inc=1, device_id={"col": lax.rem(c + d, C)}, device_id_type=MESH)

    for j in range(R):
        cols = slice(j * slab, (j + 1) * slab)
        x = expr[:, cols]
        total = jnp.sum(x, axis=0, keepdims=True)
        dev = x - total * (1.0 / S)
        stats[0, 0:1, cols] = total
        stats[0, 1:2, cols] = jnp.sum(dev * dev, axis=0, keepdims=True)
    pl.semaphore_wait(barrier, R + C - 2)

    def rowcopy(src, dst, ss, rr, d):
        return pltpu.make_async_remote_copy(
            src_ref=src, dst_ref=dst, send_sem=ss, recv_sem=rr,
            device_id={"row": flip(r, d)}, device_id_type=MESH)

    def colcopy(src, dst, ss, rr, peer):
        return pltpu.make_async_remote_copy(
            src_ref=src, dst_ref=dst, send_sem=ss, recv_sem=rr,
            device_id={"col": peer}, device_id_type=MESH)

    st = [rowcopy(stats.at[0], stats.at[d], s_st.at[d], r_st.at[d], d) for d in range(1, R)]
    for cp in st:
        cp.start()
    macc[...] = jnp.zeros_like(macc)
    zl[pad - 16:pad, :] = jnp.zeros((16, width), BF16)
    pbuf[...] = jnp.ones_like(pbuf)
    for cp in st:
        cp.wait_recv()

    for j in range(R):
        cols = slice(j * slab, (j + 1) * slab)
        total = stats[0, 0:1, cols]
        for d in range(1, R):
            total = total + stats[d, 0:1, cols]
        mean = total / (S * R)
        sq = jnp.zeros_like(mean)
        for d in range(R):
            gap = stats[d, 0:1, cols] * (1.0 / S) - mean
            sq = sq + (stats[d, 1:2, cols] + S * gap * gap)
        inv = 1.0 / jnp.sqrt(sq + eps)
        zl[0:S, cols] = ((expr[:, cols] - mean) * inv).astype(BF16)

    mine = pl.ds(pl.multiple_of(r * pad, 16), pad)
    aa = []
    for k in range(NC):
        for d in range(1, R):
            q = flip(r, d)
            at = pl.multiple_of(q * slab + k * chunk, 128)
            aa.append(rowcopy(zl.at[:, pl.ds(at, chunk)],
                              zcol.at[q, mine, k * chunk:(k + 1) * chunk],
                              s_aa.at[k, d], r_aa.at[k, d], d))
            aa[-1].start()
    zcol[r, mine, :] = zl[:, pl.ds(pl.multiple_of(r * slab, 128), slab)]

    pick = jnp.zeros((pad, W), F32)
    for j in range(R):
        gene = lax.broadcasted_iota(jnp.int32, (slab, W), 0) + (c * width + j * slab)
        onehot = jnp.where(gene == win[...], 1.0, 0.0).astype(BF16)
        pick = pick + dot(zl[:, j * slab:(j + 1) * slab], onehot)
    zw[0] = pick.astype(BF16)
    zc = []
    for d in range(1, C):
        zc.append(colcopy(zw.at[0], zw.at[d], s_zc.at[d], r_zc.at[d], lax.rem(c + d, C)))
        zc[-1].start()

    zr_own = zcol.at[r]
    lo, hi = c > 0, c < C - 1

    def up(s, k):
        i = c - s
        return colcopy(zrt.at[i, k], zrt.at[i, k], s_up.at[s, k], r_up.at[s, k], c + 1)

    def up_in(s, k):
        i = c - s
        return colcopy(zrt.at[i, k], zrt.at[i, k], s_up.at[s - 1, k], r_up.at[s - 1, k], c + 1)

    def down(s, k):
        i = c + s
        return colcopy(zrt.at[i, k], zrt.at[i, k], s_dn.at[s, k], r_dn.at[s, k], c - 1)

    def down_in(s, k):
        i = c + s
        return colcopy(zrt.at[i, k], zrt.at[i, k], s_dn.at[s - 1, k], r_dn.at[s - 1, k], c - 1)

    for k in range(NC):
        for cp in aa[k * (R - 1):(k + 1) * (R - 1)]:
            cp.wait_recv()
        zrt[c, k] = zr_own[:, k * chunk:(k + 1) * chunk].T

        @pl.when(hi)
        def _():
            up(0, k).start()

        @pl.when(lo)
        def _():
            down(0, k).start()

    relay = R == 4

    def gather(k, d):
        piece = zcol.at[r, :, pl.ds(pl.multiple_of(k * chunk, 128), chunk)]
        return rowcopy(piece, piece, s_ga.at[k, d], r_ga.at[k, d], d)

    def forward(k, via, to):
        piece = zcol.at[flip(r, via), :, pl.ds(pl.multiple_of(k * chunk, 128), chunk)]
        return rowcopy(piece, piece, s_ga.at[k, R - 1], r_ga.at[k, R - 1], to)

    direct = R - 1 if relay else R
    for d in range(1, direct):
        gather(0, d).start()

    tot = zw[0].astype(F32)
    for cp in zc:
        cp.wait_recv()
    for d in range(1, C):
        tot = tot + zw[d].astype(F32)
    zwr[0] = tot.astype(BF16)
    zr = []
    for d in range(1, R):
        zr.append(rowcopy(zwr.at[0], zwr.at[d], s_zr.at[d], r_zr.at[d], d))
        zr[-1].start()
    for k in range(1, NC):
        for d in range(1, direct):
            gather(k, d).start()
    for cp in zr:
        cp.wait_recv()
    for d in range(R):
        zwt[pl.ds(pl.multiple_of(flip(r, d) * pad, 16), pad), :] = zwr[d]

    def compute(i, k, d_lo, d_hi):
        def one(d, _):
            j = flip(r, d)
            adj = power_eight(dot(zrt[i, k], zcol[j])).astype(BF16)
            macc[j] += dot(pbuf[i, k], adj)
            return 0
        lax.fori_loop(d_lo, d_hi, one, 0)

    def panel(i, k):
        pt = power_eight(dot(zrt[i, k], zwt[...])).T
        pbuf[i, k, 0:W, :] = pt.astype(BF16)

    def arrive(s, k):
        @pl.when(c - s >= 0)
        def _():
            up_in(s, k).wait_recv()

            @pl.when(hi)
            def _():
                up(s, k).start()

        @pl.when(c + s < C)
        def _():
            down_in(s, k).wait_recv()

            @pl.when(lo)
            def _():
                down(s, k).start()

    def phase(s, t_lo, t_hi, start, d_hi):
        def step(k, _):
            arrive(s, k)

            def each(t, _):
                i = c + (1 - 2 * (t % 2)) * ((t + 1) // 2)

                @pl.when((i >= 0) & (i < C))
                def _():
                    @pl.when(start(t) == 0)
                    def _():
                        panel(i, k)
                    compute(i, k, start(t), d_hi)
                return 0
            lax.fori_loop(t_lo, t_hi, each, 0)
            return 0
        lax.fori_loop(0, NC, step, 0)

    def own(k, _):
        panel(c, k)
        compute(c, k, 0, 1)
        return 0
    lax.fori_loop(0, NC, own, 0)

    for k in range(NC):
        arrive(1, k)
        for d in range(1, R - 1):
            gather(k, d).wait_recv()
        if relay:
            via = 1 if k < NC // 2 else 2
            forward(k, via, 3 - via).start()
    phase(2, 0, 3, lambda t: jnp.where(t == 0, 1, 0), R - 1)
    for k in range(NC):
        gather(k, R - 1).wait_recv()
    phase(3, 0, 7, lambda t: jnp.where(t < 3, R - 1, 0), R)
    if C > 4:
        def later(s, _):
            phase(s, 2 * s - 1, 2 * s + 1, lambda t: 0, R)
            return 0
        lax.fori_loop(4, C, later, 0)

    out_cp = []
    for d in range(1, R):
        q = pl.multiple_of(flip(r, d) * per, 8)
        for j in range(R):
            out_cp.append(rowcopy(macc.at[j, pl.ds(q, per), :], rs.at[d, j],
                                  s_rs.at[d, j], r_rs.at[d, j], d))
            out_cp[-1].start()
    for j in range(R):
        degb[j] = macc[j, W:W + 1, :]
    zs = zcol[r].astype(F32)
    self_term = power_eight(jnp.sum(zs * zs, axis=0, keepdims=True))
    degb[r] = degb[r] - self_term.astype(BF16).astype(F32)
    dg = []
    for d in range(1, R):
        dg.append(rowcopy(degb, degr.at[d], s_dg.at[d], r_dg.at[d], d))
        dg[-1].start()
    own_rows = pl.ds(pl.multiple_of(r * per, 8), per)
    for j in range(R):
        total = macc[j, own_rows, :]
        for d in range(1, R):
            out_cp[(d - 1) * R + j].wait_recv()
            total = total + rs[d, j]
        out[:, j * slab:(j + 1) * slab] = total
    for cp in dg:
        cp.wait_recv()
    for j in range(R):
        total = degb[j]
        for d in range(1, R):
            total = total + degr[d, j]
        dego[:, j * slab:(j + 1) * slab] = total

    for cp in st + aa + zc + zr + out_cp + dg:
        cp.wait_send()
    for k in range(NC):
        for d in range(1, R):
            gather(k, d).wait_send()

    def drain(s, _):
        def each(k, _):
            @pl.when(hi & (c - s >= 0))
            def _():
                up(s, k).wait_send()

            @pl.when(lo & (c + s < C))
            def _():
                down(s, k).wait_send()
            return 0
        lax.fori_loop(0, NC, each, 0)
        return 0
    lax.fori_loop(0, C - 1, drain, 0)


LIMIT = 65535.0


def quantize(v):
    h = v.shape[0] // 2
    top = jnp.maximum(jnp.max(v, axis=0, keepdims=True), 1e-20)
    inv = LIMIT / top
    code = (v * inv + 0.5).astype(jnp.int32)
    return code[:h] | lax.shift_left(code[h:], 16), top


def restore(code, top):
    unit = top * (1.0 / LIMIT)
    low = (code & 65535).astype(F32) * unit
    high = lax.shift_right_logical(code, 16).astype(F32) * unit
    return low, high


def gather_plan():
    plan = {}
    for d in (1, 2):
        e, sent, groups = d - 1, set(), []
        for m in range(4):
            group = []
            for piece in [(3 ^ m, e), (d ^ m, e), (d ^ m, 1 - e)]:
                if piece not in sent:
                    sent.add(piece)
                    group.append(piece)
            groups.append(group)
        plan[d] = groups
    return plan


def folded_kernel(eps, expr, win, out, dego,
                  stats, zcol, zf, zt, zw, zwr, zwt, zwn, pcol, prow, macc, ret,
                  rtq, rta, rbq, rba, rsq, rsa, rbufq, rbufa, degb, degr,
                  s_st, r_st, s_ag, r_ag, s_rl, s_z, r_z, s_zf, s_zc, r_zc, s_zr, r_zr,
                  s_rt, r_rt, s_rs, r_rs, s_dg, r_dg):
    R, C = 4, 4
    t = lax.axis_index("tissue")
    r = lax.axis_index("row")
    c = lax.axis_index("col")
    p = c + t * (C - 1 - 2 * c)
    S, width = expr.shape
    slab = width // R
    half = slab // 2
    pad = zcol.shape[1] // R
    W = zw.shape[2]
    per = W // R
    CH = zt.shape[1] // 2
    full = (S + 7) // 8 * 8

    def block(d):
        return slice(d * pad, d * pad + full)

    def rowpeer(d):
        return {"row": flip(r, d)}

    def colpeer(q):
        return {"col": q + t * (C - 1 - 2 * q)}

    def copy(src, dst, ss, rr, dev):
        return pltpu.make_async_remote_copy(
            src_ref=src, dst_ref=dst, send_sem=ss, recv_sem=rr,
            device_id=dev, device_id_type=MESH)

    started = []

    def send(src, dst, ss, rr, dev):
        cp = copy(src, dst, ss, rr, dev)
        cp.start()
        started.append(cp)

    def arrived(dst, rr):
        copy(dst, dst, rr, rr, rowpeer(1)).wait_recv()

    for d in range(R):
        tail = slice((d + 1) * pad - 16, (d + 1) * pad)
        for m in range(R):
            zcol[m, tail, :] = jnp.zeros((16, slab), BF16)
        for f in range(2):
            zf[f, tail, :] = jnp.zeros((16, slab), BF16)

    barrier = pltpu.get_barrier_semaphore()
    for d in range(1, R):
        pl.semaphore_signal(barrier, inc=1, device_id=rowpeer(d), device_id_type=MESH)
    for d in range(1, C):
        pl.semaphore_signal(barrier, inc=1, device_id={"col": lax.rem(c + d, C)}, device_id_type=MESH)

    def at(m):
        return pl.ds(pl.multiple_of(flip(r, m) * slab, 128), slab)

    for j in range(R):
        cols = slice(j * slab, (j + 1) * slab)
        x = expr[:, cols]
        total = jnp.sum(x, axis=0, keepdims=True)
        dev = x - total * (1.0 / S)
        stats[0, 0:1, cols] = total
        stats[0, 1:2, cols] = jnp.sum(dev * dev, axis=0, keepdims=True)
    pl.semaphore_wait(barrier, R + C - 2)
    for d in range(1, R):
        send(stats.at[0], stats.at[d], s_st.at[d], r_st.at[d], rowpeer(d))
    for m in range(R):
        macc[m] = jnp.zeros(macc.shape[1:], F32)
        pcol[m, W:, :] = jnp.ones((16, slab), BF16)
    for f in range(2):
        prow[f, W:, :] = jnp.ones((16, slab), BF16)
        ret[f] = jnp.zeros(ret.shape[1:], F32)
    for d in range(1, R):
        arrived(stats.at[d], r_st.at[d])

    plan = gather_plan()

    def direct(d, g):
        for rel, e in plan[d][g]:
            cols = slice(e * half, (e + 1) * half)
            send(zcol.at[rel, block(0), cols], zcol.at[rel ^ d, block(d), cols],
                 s_ag.at[d, rel, e], r_ag.at[d, rel ^ d, e], rowpeer(d))

    seen = set()

    def landed(d, m, e):
        if (d, m, e) in seen:
            return
        seen.add((d, m, e))
        cols = slice(e * half, (e + 1) * half)
        arrived(zcol.at[m, block(d), cols], r_ag.at[d, m, e])

    def relay(g, links=(1, 2)):
        for d in links:
            n, e = 3 - d, 2 - d
            rel = d ^ g
            cols = slice(e * half, (e + 1) * half)
            landed(n, rel, e)
            send(zcol.at[rel, block(n), cols], zcol.at[g, block(3), cols],
                 s_rl.at[d, g], r_ag.at[3, g, e], rowpeer(d))

    def gathered(m):
        for d in range(1, R):
            for e in range(2):
                landed(d, m, e)

    for m in (3, 1, 2, 0):
        cols = at(m)
        total = stats[0, 0:1, cols]
        for d in range(1, R):
            total = total + stats[d, 0:1, cols]
        mean = total / (S * R)
        sq = jnp.zeros_like(mean)
        for d in range(R):
            gap = stats[d, 0:1, cols] * (1.0 / S) - mean
            sq = sq + (stats[d, 1:2, cols] + S * gap * gap)
        inv = 1.0 / jnp.sqrt(sq + eps)
        zcol[m, 0:S, :] = ((expr[:, cols] - mean) * inv).astype(BF16)
        if m == 2:
            for d in (1, 2):
                direct(d, 0)

    zslot = p // 3
    zpeer = colpeer(jnp.where(p == 3, 1, p + 1))

    def zsend_copy(d):
        rows = block(d)
        return copy(zcol.at[0, rows, :], zf.at[zslot, rows, :], s_z.at[d], r_z.at[zslot, d], zpeer)

    def zsend(ds, cond):
        @pl.when(cond)
        def _():
            for d in ds:
                zsend_copy(d).start()

    pick = jnp.zeros((pad, W), F32)
    for m in range(R):
        gene = lax.broadcasted_iota(jnp.int32, (slab, W), 0) + (c * width + flip(r, m) * slab)
        onehot = jnp.where(gene == win[...], 1.0, 0.0).astype(BF16)
        pick = pick + dot(zcol[m, 0:pad, :], onehot)
    zw[0] = pick.astype(BF16)
    for d in range(1, C):
        send(zw.at[0], zw.at[d], s_zc.at[d], r_zc.at[d], {"col": lax.rem(c + d, C)})
    zsend((0,), p >= 0)

    relay(0)
    tot = zw[0].astype(F32)
    for d in range(1, C):
        arrived(zw.at[d], r_zc.at[d])
        tot = tot + zw[d].astype(F32)
    zwr[0] = tot.astype(BF16)
    for d in range(1, R):
        send(zwr.at[0], zwr.at[d], s_zr.at[d], r_zr.at[d], rowpeer(d))
    for d in (1, 2):
        direct(d, 1)
    for d in range(1, R):
        for e in range(2):
            landed(d, 0, e)
        zsend((d,), p < 3)

    zt[0] = zcol[0].T
    for d in range(1, R):
        arrived(zwr.at[d], r_zr.at[d])
    for d in range(R):
        zwt[d * pad:(d + 1) * pad, :] = zwr[d]
    zwn[...] = zwt[...].T

    def panel_col(m):
        pcol[m, 0:W, :] = power_eight(dot(zwn[...], zcol[m])).astype(BF16)

    def chunk(k):
        return pl.ds(pl.multiple_of(k * CH, 128), CH)

    def own(m):
        def step(k, _):
            rows = chunk(k)
            adj = power_eight(dot(zt[0, rows, :], zcol[m])).astype(BF16)
            macc[m] += dot(pcol[0, :, rows], adj)
            return 0
        lax.fori_loop(0, 2, step, 0)

    def cross(f, k, m):
        rows = chunk(k)
        adj = power_eight(dot(zt[1 + f, rows, :], zcol[m])).astype(BF16)
        macc[m] += dot(prow[f, :, rows], adj)
        ret[f, :, rows] += dot(pcol[m], adj, ((1,), (1,)))

    def crosses(f, m_lo, m_hi):
        def step(i, _):
            cross(f, lax.rem(i, 2), m_lo + i // 2)
            return 0
        lax.fori_loop(0, 2 * (m_hi - m_lo), step, 0)

    def prepare(f):
        zt[1 + f] = zf[f].T
        prow[f, 0:W, :] = power_eight(dot(zwn[...], zf[f])).astype(BF16)

    def zwait(f, ds):
        for d in ds:
            arrived(zf.at[f, block(d), :], r_z.at[f, d])

    def zrelay_copy(f, d):
        rows = block(d)
        return copy(zf.at[f, rows, :], zf.at[1, rows, :], s_zf.at[f, d], r_z.at[1, d], colpeer(2 + f))

    def zrelay(f, ds):
        @pl.when(p == 1 + f)
        def _():
            for d in ds:
                zwait(f, (d,))
                zrelay_copy(f, d).start()

    def back_copies(f, k):
        cols = slice(k * CH, (k + 1) * CH)
        if f == 0:
            dest, slot = p - 1, 0
        else:
            dest, slot = jnp.where(p == 1, 3, 0), p - 1
        made = []
        for d in (3, 1, 2, 0):
            dev = {**colpeer(dest), **(rowpeer(d) if d else {})}
            made += [copy(rtq.at[f, d, :, cols], rbq.at[slot, d, :, cols],
                          s_rt.at[f, k, d, 0], r_rt.at[slot, k, d, 0], dev),
                     copy(rta.at[f, k, d], rba.at[slot, k, d],
                          s_rt.at[f, k, d, 1], r_rt.at[slot, k, d, 1], dev)]
        return made

    def give_back(f, k):
        cols = slice(k * CH, (k + 1) * CH)
        made = back_copies(f, k)
        for i, d in enumerate((3, 1, 2, 0)):
            rows = pl.ds(pl.multiple_of(flip(r, d) * per, 8), per)
            code, top = quantize(ret[f, rows, cols])
            rtq[f, d, :, cols] = code
            rta[f, k, d, 0:1, :] = top
            rta[f, k, d, 1:2, :] = ret[f, W:W + 1, cols]
            made[2 * i].start()
            made[2 * i + 1].start()

    def take_back(slot):
        for k in range(2):
            cols = slice(k * CH, (k + 1) * CH)
            for m in range(R):
                arrived(rbq.at[slot, m, :, cols], r_rt.at[slot, k, m, 0])
                arrived(rba.at[slot, k, m], r_rt.at[slot, k, m, 1])
                there = pl.ds(pl.multiple_of(flip(r, m) * slab + k * CH, 128), CH)
                low, high = restore(rbq[slot, m, :, cols], rba[slot, k, m, 0:1, :])
                out[0:hp, there] += low
                out[hp:per, there] += high
                dego[:, there] += rba[slot, k, m, 1:2, :]

    def scatter_copies(m):
        made = []
        for d in (3, 1, 2):
            made += [copy(rsq.at[d, m], rbufq.at[d, m ^ d], s_rs.at[d, m, 0], r_rs.at[d, m ^ d, 0], rowpeer(d)),
                     copy(rsa.at[d, m], rbufa.at[d, m ^ d], s_rs.at[d, m, 1], r_rs.at[d, m ^ d, 1], rowpeer(d))]
        return made

    def scatter(m):
        made = scatter_copies(m)
        for i, d in enumerate((3, 1, 2)):
            rows = pl.ds(pl.multiple_of(flip(r, d) * per, 8), per)
            code, top = quantize(macc[m, rows, :])
            rsq[d, m] = code
            rsa[d, m] = top
            made[2 * i].start()
            made[2 * i + 1].start()

    away = p >= 1
    hp = per // 2

    panel_col(0)
    own(0)
    relay(1)
    for d in (1, 2):
        direct(d, 2)
        direct(d, 3)
    zrelay(0, range(R))

    @pl.when(p >= 2)
    def _():
        zwait(0, range(R))

    @pl.when(away)
    def _():
        prepare(0)
        crosses(0, 0, 1)
    gathered(1)
    relay(2)
    panel_col(1)
    own(1)
    relay(3)
    zrelay(1, (0,))

    @pl.when(away)
    def _():
        crosses(0, 1, 2)
    zrelay(1, (1, 2))
    gathered(2)
    zsend((1, 2, 3), p == 3)
    panel_col(2)
    zrelay(1, (3,))
    own(2)
    gathered(3)
    panel_col(3)
    for k in range(2):
        @pl.when(away)
        def _():
            lax.fori_loop(2, R, lambda m, _: (cross(0, k, m), 0)[1], 0)
            give_back(0, k)

    @pl.when((p == 1) | (p == 3))
    def _():
        zwait(1, range(R))

    @pl.when(away)
    def _():
        prepare(1)
    for m in range(2):
        @pl.when(away)
        def _():
            crosses(1, m, m + 1)
        scatter(m)

    @pl.when(away)
    def _():
        for k in range(2):
            lax.fori_loop(2, R, lambda m, _: (cross(1, k, m), 0)[1], 0)
            give_back(1, k)
    scatter(2)
    own(3)
    scatter(3)

    zs = zcol[0].astype(F32)
    self_term = power_eight(jnp.sum(zs * zs, axis=0, keepdims=True))
    for m in range(R):
        degb[m] = macc[m, W:W + 1, :]
    degb[0] = degb[0] - self_term.astype(BF16).astype(F32)
    for d in range(1, R):
        send(degb, degr.at[d], s_dg.at[d], r_dg.at[d], rowpeer(d))

    mine = pl.multiple_of(r * per, 8)
    for m in range(R):
        for q in range(2):
            acc = macc[m, pl.ds(mine + q * hp, hp), :]
            for d in range(1, R):
                if q == 0:
                    arrived(rbufq.at[d, m], r_rs.at[d, m, 0])
                    arrived(rbufa.at[d, m], r_rs.at[d, m, 1])
                acc = acc + restore(rbufq[d, m], rbufa[d, m])[q]
            out[q * hp:(q + 1) * hp, at(m)] = acc
    for d in range(1, R):
        arrived(degr.at[d], r_dg.at[d])
    for m in range(R):
        total = degb[m]
        for d in range(1, R):
            total = total + degr[d, m ^ d]
        dego[:, at(m)] = total
    take_back(0)

    @pl.when(p == 0)
    def _():
        take_back(1)
        take_back(2)

    for cp in started:
        cp.wait_send()
    for m in range(R):
        for cp in scatter_copies(m):
            cp.wait_send()

    for d in range(R):
        zsend_copy(d).wait_send()

    for f in range(2):
        @pl.when(p == 1 + f)
        def _():
            for d in range(R):
                zrelay_copy(f, d).wait_send()

    @pl.when(away)
    def _():
        for f in range(2):
            for k in range(2):
                for cp in back_copies(f, k):
                    cp.wait_send()


def folded(expr, win):
    R = C = 4
    S, width = expr.shape
    W = win.shape[0]
    pad = (S + 15) // 16 * 16
    slab = width // R
    V = pltpu.VMEM
    I32 = jnp.int32
    dma = pltpu.SemaphoreType.DMA
    vm = pl.BlockSpec(memory_space=pltpu.VMEM)
    half = slab // 2
    margin, degree = pl.pallas_call(
        functools.partial(folded_kernel, 1e-6),
        out_shape=(jax.ShapeDtypeStruct((W // R, width), F32),
                   jax.ShapeDtypeStruct((1, width), F32)),
        in_specs=[vm, vm],
        out_specs=(vm, vm),
        scratch_shapes=[
            V((R, 2, width), F32),
            V((R, R * pad, slab), BF16),
            V((2, R * pad, slab), BF16),
            V((3, slab, R * pad), BF16),
            V((C, pad, W), BF16),
            V((R, pad, W), BF16),
            V((R * pad, W), BF16),
            V((W, R * pad), BF16),
            V((R, W + 16, slab), BF16),
            V((2, W + 16, slab), BF16),
            V((R, W + 16, slab), F32),
            V((2, W + 16, slab), F32),
            V((2, R, W // R // 2, slab), I32),
            V((2, 2, R, 2, half), F32),
            V((3, R, W // R // 2, slab), I32),
            V((3, 2, R, 2, half), F32),
            V((R, R, W // R // 2, slab), I32),
            V((R, R, 1, slab), F32),
            V((R, R, W // R // 2, slab), I32),
            V((R, R, 1, slab), F32),
            V((R, 1, slab), F32),
            V((R, R, 1, slab), F32),
            dma((R,)), dma((R,)),
            dma((R, R, 2)), dma((R, R, 2)), dma((R, R)),
            dma((R,)), dma((2, R)), dma((2, R)),
            dma((C,)), dma((C,)), dma((R,)), dma((R,)),
            dma((2, 2, R, 2)), dma((3, 2, R, 2)),
            dma((R, R, 2)), dma((R, R, 2)),
            dma((R,)), dma((R,)),
        ],
        compiler_params=pltpu.CompilerParams(
            collective_id=0, has_side_effects=True, vmem_limit_bytes=46 << 20),
    )(expr, win.reshape(1, W))
    return margin, degree.reshape(width)


def solution(mesh):
    R, C = mesh.shape["row"], mesh.shape["col"]

    def body(expr, win):
        if R == 4 and C == 4:
            return folded(expr, win)
        S, width = expr.shape
        W = win.shape[0]
        pad = (S + 15) // 16 * 16
        slab = width // R
        chunk = min(256, slab)
        NC = slab // chunk
        V = pltpu.VMEM
        dma = pltpu.SemaphoreType.DMA
        vm = pl.BlockSpec(memory_space=pltpu.VMEM)
        margin, degree = pl.pallas_call(
            functools.partial(kernel, R, C, 1e-6),
            out_shape=(jax.ShapeDtypeStruct((W // R, width), F32),
                       jax.ShapeDtypeStruct((1, width), F32)),
            in_specs=[vm, vm],
            out_specs=(vm, vm),
            scratch_shapes=[
                V((R, 2, width), F32),
                V((pad, width), BF16),
                V((R, R * pad, slab), BF16),
                V((C, NC, chunk, R * pad), BF16),
                V((C, pad, W), BF16),
                V((R, pad, W), BF16),
                V((R * pad, W), BF16),
                V((C, NC, W + 16, chunk), BF16),
                V((R, W + 16, slab), F32),
                V((R, R, W // R, slab), F32),
                V((R, 1, slab), F32),
                V((R, R, 1, slab), F32),
                dma((R,)), dma((R,)), dma((NC, R)), dma((NC, R)), dma((NC, R)), dma((NC, R)),
                dma((C,)), dma((C,)), dma((R,)), dma((R,)),
                dma((C, NC)), dma((C, NC)), dma((C, NC)), dma((C, NC)),
                dma((R, R)), dma((R, R)), dma((R,)), dma((R,)),
            ],
            compiler_params=pltpu.CompilerParams(
                collective_id=0, has_side_effects=True, vmem_limit_bytes=56 << 20),
        )(expr, win.reshape(1, W))
        return margin, degree.reshape(width)

    in_specs = (P(("tissue", "row"), "col"), P())
    out_specs = (P(("tissue", "row"), "col"), P(("tissue", "col")))
    return jax.shard_map(body, mesh=mesh, in_specs=in_specs, out_specs=out_specs, check_vma=False)
```
